32 devices in a mesh: dof: 16 (over z, x, core), mode: 2 (over y).
Axes of the slice: x: 2, y: 2, z: 4, core: 2. Of those that a mesh axis runs over, the one named last changes fastest.
Arguments:
- stiffness_tiles: bfloat16 [512, 10, 128, 128], P('dof'), may hold values from -0.15625 to 0.15625
- tile_cols: int32 [512, 10], P('dof'), may hold values from 0 to 47, as said below
- send_rows: int32 [32, 8], P('dof'), may hold values from 0 to 31, as said below
- block: bfloat16 [65536, 128], P('dof', 'mode'), may hold values from -51 to 51
- lower_bound: float32 [1], replicated, may hold values from -1.2 to -0.6
- upper_bound: float32 [1], replicated, may hold values from 0.4 to 0.9
Outputs:
- basis: bfloat16 [65536, 128], P('dof', 'mode')
- ritz: float32 [128, 128], replicated
The draws below stay inside these ranges and needn't reach their ends.
Inputs may be any that keep to these rules, and one draw needn't show every extreme that they name: `tile_cols`: entry 0 of every tile row is that row's own local index; entry 1 is a code of the lower neighbour's upward list and entry 2 a code of the upper neighbour's downward list. A code below 32 is a tile row of the same partition; 32 + s is slot s of the lower neighbour's upward list; 40 + s is slot s of the upper neighbour's downward list. `send_rows`: rows 2 p and 2 p + 1 hold distinct local tile rows of partition p: its downward and upward send lists.
All inputs are finite; a program needn't handle non-finite values.
Results may differ from the reference program's by a relative error of at most 0.0086.
Values may be sent and summed in bfloat16 or wider, within the bound.
A program may use at most 64 MiB of HBM per device.

```python
import jax
import jax.numpy as jnp
from jax import lax

TILE = 128
MODES = 128
NNZ = 10
DEGREE = 2
ROWT = 32
NSEND = 8
TROWS = 512
NDOF = 65536


def draw_block(key, part):
    key_base = jax.random.fold_in(key, 0)
    key_common = jax.random.fold_in(key, 2)
    key_weights = jax.random.fold_in(key, 3)
    shared_count = 8
    row_index = jnp.arange(NDOF, dtype=jnp.float32)[:, None]
    row_rise = 1.0 + 2.0 * row_index / NDOF
    mixing = jnp.clip(jax.random.normal(key_weights, (shared_count, MODES), jnp.float32), -4.0, 4.0)
    base_draw = jnp.clip(jax.random.normal(key_base, (NDOF, MODES), jnp.float32), -6.0, 6.0)
    common = jnp.clip(jax.random.normal(key_common, (NDOF, shared_count), jnp.float32), -4.0, 4.0)
    shared = 0.45 * jnp.dot(common, mixing, precision=lax.Precision.HIGHEST)
    values = (base_draw + shared) * row_rise
    return jnp.clip(values, -51.0, 51.0).astype(jnp.bfloat16)


def draw_tile_cols(key, part):
    key_pick, key_local, key_ghost, key_low, key_up = jax.random.split(key, 5)
    local_col = jax.random.randint(key_local, (TROWS, NNZ), 0, ROWT)
    ghost_col = jax.random.randint(key_ghost, (TROWS, NNZ), ROWT, ROWT + 2 * NSEND)
    chooser = jax.random.randint(key_pick, (TROWS, NNZ), 0, 10)
    picked = jnp.where(chooser < 3, ghost_col, local_col)
    low_col = jax.random.randint(key_low, (TROWS, NNZ), ROWT, ROWT + NSEND)
    up_col = jax.random.randint(key_up, (TROWS, NNZ), ROWT + NSEND, ROWT + 2 * NSEND)
    own_row = (jnp.arange(TROWS, dtype=jnp.int32) % ROWT)[:, None]
    column = jnp.arange(NNZ, dtype=jnp.int32)[None, :]
    picked = jnp.where(column == 1, low_col, jnp.where(column == 2, up_col, picked))
    return jnp.where(column == 0, own_row, picked).astype(jnp.int32)


def draw_send_rows(key, part):
    list_count = 2 * (TROWS // ROWT)
    scores = jax.random.randint(key, (list_count, ROWT), 0, 1 << 20) * ROWT + jnp.arange(ROWT, dtype=jnp.int32)[None, :]
    ordering = jnp.argsort(scores, axis=-1, stable=True)
    return ordering[:, :NSEND].astype(jnp.int32)


def shard_levels(key, shape, cuts, least, high):
    level, own = 1.0, jax.random.fold_in(key, 6)
    for dim, shards_of in cuts:
        heights = jnp.exp(jax.random.uniform(jax.random.fold_in(own, dim), (shards_of,), jnp.float32, least / len(cuts), high / len(cuts)))
        level = level * jnp.repeat(heights, shape[dim] // shards_of).reshape([-1 if axis == dim else 1 for axis in range(len(shape))])
    return level


def noise(rng, dims, width, reach, cuts=(), held_as=jnp.bfloat16):
    loudness = shard_levels(rng, dims, cuts, -0.22, 0.18) if cuts else 1.0
    values = jax.random.normal(rng, dims, jnp.float32) * width * loudness
    return jnp.minimum(jnp.maximum(values, -reach), reach).astype(held_as)


def setup_inputs(seed: int = 0) -> dict:
    splits = jax.random.split(jax.random.key(seed), 7)
    return {
        "stiffness_tiles": noise(splits[0], (TROWS, NNZ, TILE, TILE), (NNZ * TILE) ** -0.5, 0.15625, ((0, 16),)),
        "tile_cols": draw_tile_cols(jax.random.fold_in(splits[6], 71), 0),
        "send_rows": draw_send_rows(jax.random.fold_in(splits[6], 71), 0),
        "block": draw_block(jax.random.fold_in(splits[6], 71), 0),
        "lower_bound": jnp.clip(jax.random.uniform(splits[4], (1,), jnp.float32, -1.2, -0.6), -1.2, -0.6),
        "upper_bound": jnp.clip(jax.random.uniform(splits[5], (1,), jnp.float32, 0.4, 0.9), 0.4, 0.9),
    }


def apply_stiffness(stiffness_tiles, tile_cols, send_rows, field):
    part_count = TROWS // ROWT
    tile_view = field.reshape(TROWS, TILE, MODES)

    def partition_product(part_index):
        col_code = lax.dynamic_slice_in_dim(tile_cols, part_index * ROWT, ROWT, 0)
        lower_part = jnp.maximum(part_index - 1, 0).astype(jnp.int32)
        upper_part = jnp.minimum(part_index + 1, part_count - 1).astype(jnp.int32)
        low_rows = lax.dynamic_index_in_dim(send_rows, 2 * lower_part + 1, 0, keepdims=False)
        up_rows = lax.dynamic_index_in_dim(send_rows, 2 * upper_part, 0, keepdims=False)
        low_slot = jnp.clip(col_code - ROWT, 0, NSEND - 1)
        up_slot = jnp.clip(col_code - ROWT - NSEND, 0, NSEND - 1)
        source_row = jnp.where(col_code < ROWT, part_index * ROWT + col_code, jnp.where(col_code < ROWT + NSEND, lower_part * ROWT + low_rows[low_slot], upper_part * ROWT + up_rows[up_slot])).astype(jnp.int32)
        present = jnp.where(col_code < ROWT, True, jnp.where(col_code < ROWT + NSEND, part_index > 0, part_index < part_count - 1))
        blocks = tile_view[source_row].astype(jnp.float32) * present[:, :, None, None].astype(jnp.float32)
        row_tiles = lax.dynamic_slice_in_dim(stiffness_tiles, part_index * ROWT, ROWT, 0).astype(jnp.float32)
        return jnp.einsum('rkij,rkjm->rim', row_tiles, blocks)
    result = lax.map(partition_product, jnp.arange(part_count, dtype=jnp.int32))
    return result.reshape(NDOF, MODES)

def reference(stiffness_tiles, tile_cols, send_rows, block, lower_bound, upper_bound):
    center = (upper_bound[0] + lower_bound[0]) * 0.5
    half_width = (upper_bound[0] - lower_bound[0]) * 0.5
    previous = block
    current = ((apply_stiffness(stiffness_tiles, tile_cols, send_rows, block) - center * block.astype(jnp.float32)) / half_width).astype(jnp.bfloat16)
    for step in range(DEGREE - 1):
        following = (2.0 * (apply_stiffness(stiffness_tiles, tile_cols, send_rows, current) - center * current.astype(jnp.float32)) / half_width - previous.astype(jnp.float32)).astype(jnp.bfloat16)
        previous, current = (current, following)
    filtered = current
    image_block = apply_stiffness(stiffness_tiles, tile_cols, send_rows, filtered).astype(jnp.bfloat16)
    gram_matrix = jnp.dot(filtered.T.astype(jnp.float32), filtered.astype(jnp.float32), preferred_element_type=jnp.float32) / NDOF
    projected = jnp.dot(filtered.T.astype(jnp.float32), image_block.astype(jnp.float32), preferred_element_type=jnp.float32) / NDOF
    factor = jnp.linalg.cholesky(gram_matrix)
    identity = jnp.eye(MODES, dtype=jnp.float32)
    inverse = jax.scipy.linalg.solve_triangular(factor, identity, lower=True)
    ritz_matrix = jnp.dot(jnp.dot(inverse, projected, precision=lax.Precision.HIGHEST), inverse.T, precision=lax.Precision.HIGHEST)
    right_factor = inverse.T.astype(jnp.bfloat16)
    basis_out = jnp.dot(filtered.astype(jnp.float32), right_factor.astype(jnp.float32), preferred_element_type=jnp.float32).astype(jnp.bfloat16)
    return (basis_out, ritz_matrix)
```

```python
import functools

import jax
import jax.numpy as jnp
from jax import lax
from jax.experimental import pallas as pl
from jax.experimental.pallas import tpu as pltpu
from jax.sharding import PartitionSpec as P

MESH = pl.DeviceIdType.MESH
GROUP = 16
NT = (((1,), (1,)), ((), ()))
NN = (((1,), (0,)), ((), ()))
TN = (((0,), (0,)), ((), ()))
EXACT = lax.Precision.HIGHEST


def kernel(
    parts, cols, rows, low_ref, high_ref, x_hbm, a_hbm, basis_ref, ritz_ref,
    a_ref, turned, level0, level1, level2, x_ref, plain, image, other, sends, ar_send, ar_recv,
    whole, final_send, final_recv, work, inv_ref, inv_t,
    x_sem, a_sem, halo_send, halo_recv, mode_send, mode_recv, ar_ssem, ar_rsem,
):
    tiles, nnz, size = a_ref.shape[0], a_ref.shape[1], a_ref.shape[2]
    modes = x_hbm.shape[0]
    width = 2 * modes
    slots = rows.shape[1]
    stages = ar_send.shape[0] - 1
    chunks = mode_send.shape[0]
    part_rows = tiles // chunks
    p = lax.axis_index("dof")
    my = lax.axis_index("mode")
    has_low = p > 0
    has_up = p < parts - 1

    odd = lax.rem(p, 2)
    mate = p + 1 - 2 * odd
    far = p - 1 + 2 * odd
    has_far = (far >= 0) & (far < parts)
    far_slot = lax.rem(far + parts, parts)

    def flipped(bit):
        return p + bit * (1 - 2 * ((p // bit) % 2))

    barrier = pltpu.get_barrier_semaphore()
    for s in range(stages):
        pl.semaphore_signal(barrier, inc=1, device_id=(flipped(1 << s), my), device_id_type=MESH)
    pl.semaphore_signal(barrier, inc=1, device_id=(p, 1 - my), device_id_type=MESH)

    @pl.when(has_far)
    def _():
        pl.semaphore_signal(barrier, inc=1, device_id=(far_slot, my), device_id_type=MESH)

    fetch = pltpu.make_async_copy(x_hbm, x_ref, x_sem.at[0])
    fetch.start()
    fetch.wait()
    loads = []
    a_parts = a_sem.shape[0]
    share = tiles // a_parts
    for i in range(a_parts):
        span = pl.ds(i * share, share)
        loads.append(pltpu.make_async_copy(a_hbm.at[span], a_ref.at[span], a_sem.at[i]))
        loads[-1].start()

    for t in range(tiles):
        plain[t] = x_ref[:, t * size : (t + 1) * size]
    for s in range(slots):
        for which, row in enumerate((rows[odd, s], rows[1 - odd, s])):
            sends[0, which, s] = plain[row]

    @pl.when(p == 0)
    def _():
        for level in (level0, level1, level2):
            level[tiles : tiles + slots] = jnp.zeros((slots, modes, size), jnp.bfloat16)

    @pl.when(p == parts - 1)
    def _():
        for level in (level0, level1, level2):
            level[tiles + slots :] = jnp.zeros((slots, modes, size), jnp.bfloat16)

    pl.semaphore_wait(barrier, stages + 1 + has_far.astype(jnp.int32))

    def halo(index, level, remote):
        hop = odd if remote else 1 - odd
        return pltpu.make_async_remote_copy(
            src_ref=sends.at[index, 0 if remote else 1],
            dst_ref=level.at[pl.ds(tiles + slots * (1 - hop), slots)],
            send_sem=halo_send.at[index, 0 if remote else 1],
            recv_sem=halo_recv.at[index, 0 if remote else 1],
            device_id=(far_slot if remote else mate, my),
            device_id_type=MESH,
        )

    def start_far(index, level):
        pl.when(has_far)(halo(index, level, True).start)

    def start_near(index, level):
        halo(index, level, False).start()

    def wait_halo(index, level):
        near, remote = halo(index, level, False), halo(index, level, True)
        near.wait_recv()
        near.wait_send()
        pl.when(has_far)(remote.wait_recv)
        pl.when(has_far)(remote.wait_send)

    start_far(0, level0)
    start_near(0, level0)
    for t in range(tiles):
        level0[t] = plain[t]

    center = (high_ref[0] + low_ref[0]) * 0.5
    half_width = (high_ref[0] - low_ref[0]) * 0.5
    scale = jnp.ones((1, size), jnp.float32) / jnp.full((1, size), half_width, jnp.float32)

    def product(level, t):
        field = jnp.concatenate([level[cols[k, t]] for k in range(nnz)], axis=1)
        return lax.dot_general(field, turned[t], NN, preferred_element_type=jnp.float32)

    def first(t):
        own = level0[t].astype(jnp.float32)
        return ((product(level0, t) - center * own) * scale).astype(jnp.bfloat16)

    def second(t):
        own = level1[t].astype(jnp.float32)
        before = level0[t].astype(jnp.float32)
        return (2.0 * (product(level1, t) - center * own) * scale - before).astype(jnp.bfloat16)

    def send_tiles(index, which, make):
        made = [make(rows[odd if which == 0 else 1 - odd, s]) for s in range(slots)]
        for s, value in enumerate(made):
            sends[index, which, s] = value

    def all_tiles(make, target, begin, count, group=GROUP):
        group = min(group, count)

        @pl.loop(0, count // group)
        def _(i):
            made = [make(begin + i * group + u) for u in range(group)]
            for u in range(group):
                target[begin + i * group + u] = made[u]

    for i, load in enumerate(loads):
        load.wait()

        @pl.loop(0, share // 2)
        def _(j):
            for u in range(2):
                t = i * share + j * 2 + u
                for k in range(nnz):
                    turned[t, k * size : (k + 1) * size] = a_ref[t, k].T

    wait_halo(0, level0)
    send_tiles(1, 0, first)
    start_far(1, level1)
    send_tiles(1, 1, first)
    start_near(1, level1)
    all_tiles(first, level1, 0, tiles)
    wait_halo(1, level1)
    send_tiles(2, 0, second)
    start_far(2, level2)
    send_tiles(2, 1, second)
    start_near(2, level2)

    def exchange(c):
        span = pl.ds(c * part_rows, part_rows)
        return pltpu.make_async_remote_copy(
            src_ref=level2.at[span],
            dst_ref=other.at[span],
            send_sem=mode_send.at[c],
            recv_sem=mode_recv.at[c],
            device_id=(p, 1 - my),
            device_id_type=MESH,
        )

    for c in range(chunks):
        all_tiles(second, level2, c * part_rows, part_rows)
        exchange(c).start()
    wait_halo(2, level2)
    all_tiles(lambda t: product(level2, t).astype(jnp.bfloat16), image, 0, tiles)

    total = jnp.zeros((width, width), jnp.float32)
    for c in range(chunks):
        exchange(c).wait_recv()

        def accumulate(i, acc):
            left, right = [], []
            for u in range(4):
                t = c * part_rows + i * 4 + u
                left.append(jnp.concatenate([level2[t], image[t]], axis=0))
                right.append(jnp.concatenate([level2[t], other[t]], axis=0))
            return acc + lax.dot_general(
                jnp.concatenate(left, axis=1), jnp.concatenate(right, axis=1), NT,
                preferred_element_type=jnp.float32,
            )

        total = lax.fori_loop(0, part_rows // 4, accumulate, total)
    total = jnp.where(my == 1, pltpu.roll(total, modes, 1), total)

    core = lax.rem(p, 2)
    start_own = pl.multiple_of(core * modes, modes)
    start_out = pl.multiple_of((1 - core) * modes, modes)
    whole[...] = total

    def transfer(s, source, target, partner):
        copy = pltpu.make_async_remote_copy(
            src_ref=source,
            dst_ref=target,
            send_sem=ar_ssem.at[s],
            recv_sem=ar_rsem.at[s],
            device_id=partner,
            device_id_type=MESH,
        )
        copy.start()
        copy.wait()

    transfer(0, whole.at[pl.ds(start_out, modes)], ar_recv.at[0], (flipped(1), my))
    part = whole[pl.ds(start_own, modes), :] + ar_recv[0]
    for s in range(1, stages + 1):
        partner = (flipped(1 << s), my) if s < stages else (p, 1 - my)
        ar_send[s] = part
        transfer(s, ar_send.at[s], ar_recv.at[s], partner)
        if s < stages:
            part = part + ar_recv[s]
    theirs = ar_recv[stages]
    low_part = jnp.where(my == 0, part, theirs)
    high_part = jnp.where(my == 0, theirs, part)
    final_send[:modes] = low_part
    final_send[modes:] = high_part
    transfer(stages + 1, final_send, final_recv, (flipped(1), my))
    mine, received = final_send[...], final_recv[...]
    count = parts * tiles * size
    gram = jnp.where(core == 0, mine, received) / count
    projected_t = jnp.where(core == 0, received, mine) / count

    step = 16
    row_id = lax.broadcasted_iota(jnp.int32, (width, width), 0)
    col_id = lax.broadcasted_iota(jnp.int32, (width, width), 1)
    work[:, :width] = gram
    work[:, width:] = (row_id == col_id).astype(jnp.float32)
    small = lax.broadcasted_iota(jnp.int32, (step, 1), 0)
    lanes = lax.broadcasted_iota(jnp.int32, (step, width), 1)

    @pl.loop(0, width // step)
    def _(b):
        begin = pl.multiple_of(b * step, step)
        panel = work[pl.ds(begin, step), :]
        near = panel[:, :width]
        columns = [
            jnp.sum(jnp.where(lanes == begin + s, near, 0.0), axis=1, keepdims=True)
            for s in range(step)
        ]
        pivots = jnp.zeros((step, 1), jnp.float32)
        for q in range(step):
            pivot = columns[q][q : q + 1, :]
            pivots = jnp.where(small == q, pivot, pivots)
            if q == step - 1:
                break
            factor = jnp.where(small > q, columns[q] / pivot, 0.0)
            panel = panel - factor * panel[q : q + 1, :]
            for s in range(q + 1, step):
                columns[s] = columns[s] - factor * columns[s][q : q + 1, :]
        inv_ref[pl.ds(begin, step), :] = panel[:, width:] / jnp.sqrt(pivots)
        below = jnp.where(lanes >= begin + step, panel[:, :width] / pivots, 0.0)
        work[...] = work[...] - lax.dot_general(
            below, panel, TN, precision=EXACT, preferred_element_type=jnp.float32
        )

    inverse = inv_ref[...]
    half = lax.dot_general(
        inverse, projected_t, NT, precision=EXACT, preferred_element_type=jnp.float32
    )
    ritz_ref[...] = lax.dot_general(
        half, inverse, NT, precision=EXACT, preferred_element_type=jnp.float32
    )
    own = jnp.where(my == 0, inverse[:modes], pltpu.roll(inverse[modes:], modes, 1))
    inv_t[...] = own.astype(jnp.bfloat16)
    for t in range(0, tiles, 2):
        pair = jnp.concatenate(
            [jnp.concatenate([level2[u], other[u]], axis=0) for u in (t, t + 1)], axis=1
        )
        basis_ref[:, t * size : (t + 2) * size] = lax.dot_general(
            inv_t[...], pair, NN, preferred_element_type=jnp.float32
        ).astype(jnp.bfloat16)
    for c in range(chunks):
        exchange(c).wait_send()


def shards(parts, stiffness_tiles, tile_cols, send_rows, block, lower_bound, upper_bound):
    row_count, modes = block.shape
    tiles, nnz, size = stiffness_tiles.shape[:3]
    slots = send_rows.shape[1]
    width = 2 * modes
    stages = parts.bit_length() - 1
    assert 1 << stages == parts and parts > 1
    chunks = 4
    smem = pl.BlockSpec(memory_space=pltpu.SMEM)
    vmem = pl.BlockSpec(memory_space=pltpu.VMEM)
    hbm = pl.BlockSpec(memory_space=pl.ANY)
    dma = pltpu.SemaphoreType.DMA
    level = pltpu.VMEM((tiles + 2 * slots, modes, size), jnp.bfloat16)
    field = pltpu.VMEM((tiles, modes, size), jnp.bfloat16)
    basis, ritz = pl.pallas_call(
        functools.partial(kernel, parts),
        out_shape=(
            jax.ShapeDtypeStruct((modes, row_count), jnp.bfloat16),
            jax.ShapeDtypeStruct((width, width), jnp.float32),
        ),
        in_specs=[smem, smem, smem, smem, hbm, hbm],
        out_specs=(vmem, vmem),
        scratch_shapes=[
            pltpu.VMEM(stiffness_tiles.shape, jnp.bfloat16),
            pltpu.VMEM((tiles, nnz * size, size), jnp.bfloat16),
            level, level, level, pltpu.VMEM((modes, row_count), jnp.bfloat16), field, field, field,
            pltpu.VMEM((3, 2, slots, modes, size), jnp.bfloat16),
            pltpu.VMEM((stages + 1, modes, width), jnp.float32),
            pltpu.VMEM((stages + 1, modes, width), jnp.float32),
            pltpu.VMEM((width, width), jnp.float32),
            pltpu.VMEM((width, width), jnp.float32),
            pltpu.VMEM((width, width), jnp.float32),
            pltpu.VMEM((width, 2 * width), jnp.float32),
            pltpu.VMEM((width, width), jnp.float32),
            pltpu.VMEM((modes, width), jnp.bfloat16),
            dma((1,)), dma((8,)), dma((3, 2)), dma((3, 2)), dma((chunks,)), dma((chunks,)),
            dma((stages + 2,)), dma((stages + 2,)),
        ],
        compiler_params=pltpu.CompilerParams(
            collective_id=0, has_side_effects=True, vmem_limit_bytes=60 * 1024 * 1024
        ),
    )(tile_cols.T, send_rows, lower_bound, upper_bound, block.T, stiffness_tiles)
    return basis.T, ritz


def solution(mesh):
    placed = (
        P("dof", None, None, None),
        P("dof", None),
        P("dof", None),
        P("dof", "mode"),
        P(),
        P(),
    )
    return jax.shard_map(
        functools.partial(shards, mesh.shape["dof"]),
        mesh=mesh, in_specs=placed, out_specs=(P("dof", "mode"), P()), check_vma=False,
    )
```

```python
import functools

import jax
import jax.numpy as jnp
from jax import lax
from jax.experimental import pallas as pl
from jax.experimental.pallas import tpu as pltpu
from jax.sharding import PartitionSpec as P

MESH = pl.DeviceIdType.MESH
GROUP = 16
NT = (((1,), (1,)), ((), ()))
NN = (((1,), (0,)), ((), ()))
TN = (((0,), (0,)), ((), ()))
EXACT = lax.Precision.HIGHEST


def kernel(
    parts, cols, rows, low_ref, high_ref, x_hbm, a_hbm, basis_ref, ritz_ref,
    a_ref, turned, level0, level1, level2, x_ref, plain, image, other, sends,
    shares, gathered, totals, sums, work, inv_ref, inv_t,
    x_sem, a_sem, halo_send, halo_recv, mode_send, mode_recv,
    share_send, share_recv, total_send, total_recv,
):
    tiles, nnz, size = a_ref.shape[0], a_ref.shape[1], a_ref.shape[2]
    modes = x_hbm.shape[0]
    width = 2 * modes
    slots = rows.shape[1]
    chunks = mode_send.shape[0]
    p = lax.axis_index("dof")
    my = lax.axis_index("mode")
    has_low = p > 0
    has_up = p < parts - 1

    odd = lax.rem(p, 2)
    mate = p + 1 - 2 * odd
    far = p - 1 + 2 * odd
    has_far = (far >= 0) & (far < parts)
    far_slot = lax.rem(far + parts, parts)

    fetch = pltpu.make_async_copy(x_hbm, x_ref, x_sem.at[0])
    fetch.start()
    barrier = pltpu.get_barrier_semaphore()

    @pl.loop(1, 2 * parts)
    def _(d):
        peer = (lax.rem(p + d // 2, parts), lax.rem(my + d, 2))
        pl.semaphore_signal(barrier, inc=1, device_id=peer, device_id_type=MESH)

    fetch.wait()
    loads = []
    a_parts = a_sem.shape[0]
    share = tiles // a_parts
    for i in range(a_parts):
        span = pl.ds(i * share, share)
        loads.append(pltpu.make_async_copy(a_hbm.at[span], a_ref.at[span], a_sem.at[i]))
        loads[-1].start()

    for t in range(tiles):
        plain[t] = x_ref[:, t * size : (t + 1) * size]
    for s in range(slots):
        for which, row in enumerate((rows[odd, s], rows[1 - odd, s])):
            sends[0, which, s] = plain[row]

    @pl.when(p == 0)
    def _():
        for level in (level0, level1, level2):
            level[tiles : tiles + slots] = jnp.zeros((slots, modes, size), jnp.bfloat16)

    @pl.when(p == parts - 1)
    def _():
        for level in (level0, level1, level2):
            level[tiles + slots :] = jnp.zeros((slots, modes, size), jnp.bfloat16)

    pl.semaphore_wait(barrier, 2 * parts - 1)

    def halo(index, level, remote):
        hop = odd if remote else 1 - odd
        return pltpu.make_async_remote_copy(
            src_ref=sends.at[index, 0 if remote else 1],
            dst_ref=level.at[pl.ds(tiles + slots * (1 - hop), slots)],
            send_sem=halo_send.at[index, 0 if remote else 1],
            recv_sem=halo_recv.at[index, 0 if remote else 1],
            device_id=(far_slot if remote else mate, my),
            device_id_type=MESH,
        )

    def start_far(index, level):
        pl.when(has_far)(halo(index, level, True).start)

    def start_near(index, level):
        halo(index, level, False).start()

    def wait_halo(index, level):
        near, remote = halo(index, level, False), halo(index, level, True)
        near.wait_recv()
        near.wait_send()
        pl.when(has_far)(remote.wait_recv)
        pl.when(has_far)(remote.wait_send)

    start_far(0, level0)
    start_near(0, level0)
    for t in range(tiles):
        level0[t] = plain[t]

    center = (high_ref[0] + low_ref[0]) * 0.5
    half_width = (high_ref[0] - low_ref[0]) * 0.5
    scale = jnp.ones((1, size), jnp.float32) / jnp.full((1, size), half_width, jnp.float32)

    def product(level, t):
        field = jnp.concatenate([level[cols[k, t]] for k in range(nnz)], axis=1)
        return lax.dot_general(field, turned[t], NN, preferred_element_type=jnp.float32)

    def first(t):
        own = level0[t].astype(jnp.float32)
        return ((product(level0, t) - center * own) * scale).astype(jnp.bfloat16)

    def second(t):
        own = level1[t].astype(jnp.float32)
        before = level0[t].astype(jnp.float32)
        return (2.0 * (product(level1, t) - center * own) * scale - before).astype(jnp.bfloat16)

    def send_tiles(index, which, make):
        made = [make(rows[odd if which == 0 else 1 - odd, s]) for s in range(slots)]
        for s, value in enumerate(made):
            sends[index, which, s] = value

    def all_tiles(make, target, begin, count, group=GROUP):
        group = min(group, count)

        @pl.loop(0, count // group)
        def _(i):
            made = [make(begin + i * group + u) for u in range(group)]
            for u in range(group):
                target[begin + i * group + u] = made[u]

    for i, load in enumerate(loads):
        load.wait()

        @pl.loop(0, share // 2)
        def _(j):
            for u in range(2):
                t = i * share + j * 2 + u
                for k in range(nnz):
                    turned[t, k * size : (k + 1) * size] = a_ref[t, k].T

    wait_halo(0, level0)
    send_tiles(1, 0, first)
    start_far(1, level1)
    send_tiles(1, 1, first)
    start_near(1, level1)
    all_tiles(first, level1, 0, tiles)
    wait_halo(1, level1)
    half = tiles // 2
    quarter = half // 4
    pieces = [(0, quarter), (quarter, quarter), (2 * quarter, 2 * quarter)]
    pieces = [(0, *piece) for piece in pieces] + [(1, 0, half // 2), (1, half // 2, half // 2)]
    urgent = range(3)
    later = range(3, 5)

    def exchange(c, sender):
        which, offset, count = pieces[c]
        begin = (sender if which == 0 else 1 - sender) * half + offset
        span = pl.ds(begin, count)
        return pltpu.make_async_remote_copy(
            src_ref=level2.at[span],
            dst_ref=other.at[span],
            send_sem=mode_send.at[c],
            recv_sem=mode_recv.at[c],
            device_id=(p, 1 - my),
            device_id_type=MESH,
        )

    def exchanged(c):
        which, offset, count = pieces[c]
        begin = (my if which == 0 else 1 - my) * half + offset
        all_tiles(second, level2, begin, count)
        exchange(c, my).start()

    block = shares.shape[2]
    base = (parts - 8) // 2

    def owners(k):
        return [base + k + 2 * b for b in range(4)] if k < 2 else [base + b for b in range(8)]

    def owned(k):
        place = p - base
        inside = (place >= 0) & (place < 8)
        return inside & (lax.rem(place + 8, 2) == k) if k < 2 else inside

    def blocks_wait(ref, count, sem):
        view = ref.at[pl.ds(0, count)]
        pltpu.make_async_copy(view, view, sem).wait()

    def share(k, value):
        for b, owner in enumerate(owners(k)):
            shares[k, b] = value[b * block : (b + 1) * block]
        for b, owner in enumerate(owners(k)):
            copy = pltpu.make_async_remote_copy(
                src_ref=shares.at[k, b],
                dst_ref=gathered.at[k * parts + p],
                send_sem=share_send.at[k],
                recv_sem=share_recv.at[k],
                device_id=(owner, my),
                device_id_type=MESH,
            )
            pl.when(p != owner)(copy.start)

            @pl.when(p == owner)
            def _():
                gathered[k * parts + p] = shares[k, b]

    def total(k):
        count = len(owners(k))

        @pl.when(owned(k))
        def _():
            blocks_wait(gathered, parts - 1, share_recv.at[k])
            value = gathered[k * parts]
            for q in range(1, parts):
                value = value + gathered[k * parts + q]
            sums[k] = value
            slot = my * count + (p - base) // (8 // count)
            totals[k, slot] = value

            @pl.loop(1, 2 * parts)
            def _(d):
                pltpu.make_async_remote_copy(
                    src_ref=sums.at[k],
                    dst_ref=totals.at[k, slot],
                    send_sem=total_send.at[k],
                    recv_sem=total_recv.at[k],
                    device_id=(lax.rem(p + d // 2, parts), lax.rem(my + d, 2)),
                    device_id_type=MESH,
                ).start()

    def arrived(k):
        count = len(owners(k))

        @pl.when(owned(k))
        def _():
            blocks_wait(totals.at[k], 2 * count - 1, total_recv.at[k])

        @pl.when(jnp.logical_not(owned(k)))
        def _():
            blocks_wait(totals.at[k], 2 * count, total_recv.at[k])

        flat = totals[k, : 2 * count].reshape(2, count * block, width) / (parts * tiles * size)
        return flat[0], flat[1]

    def sent(k):
        count = len(owners(k))

        @pl.when(owned(k))
        def _():
            blocks_wait(shares.at[k], count - 1, share_send.at[k])
            blocks_wait(gathered, 2 * parts - 1, total_send.at[k])

        @pl.when(jnp.logical_not(owned(k)))
        def _():
            blocks_wait(shares.at[k], count, share_send.at[k])

    def contract(left, right, begin, count):
        acc = jnp.zeros((modes, modes), jnp.float32)
        for i in range(0, count, 8):
            lhs = jnp.concatenate([left[begin + i + u] for u in range(8)], axis=1)
            rhs = jnp.concatenate([right[begin + i + u] for u in range(8)], axis=1)
            acc = acc + lax.dot_general(lhs, rhs, NT, preferred_element_type=jnp.float32)
        return acc

    def fold(value):
        return jnp.concatenate([value[: modes // 2], value[modes // 2 :]], axis=1)

    def unfold(value):
        return jnp.concatenate([value[:, :modes], value[:, modes:]], axis=0)

    for c in urgent:
        exchanged(c)
    send_tiles(2, 0, second)
    start_far(2, level2)
    send_tiles(2, 1, second)
    start_near(2, level2)
    for c in later:
        exchanged(c)
    share(0, fold(contract(level2, level2, 0, tiles)))
    wait_halo(2, level2)
    all_tiles(lambda t: product(level2, t).astype(jnp.bfloat16), image, 0, tiles)
    for c in urgent:
        exchange(c, 1 - my).wait_recv()
    cross = contract(level2, other, (1 - my) * half, half)
    share(1, fold(jnp.where(my == 0, cross, cross.T)))
    total(0)
    own_projected = contract(image, level2, 0, tiles)
    mixed = contract(image, other, (1 - my) * half, half)
    total(1)
    for c in later:
        exchange(c, 1 - my).wait_recv()
    mixed = mixed + contract(image, other, my * half, half)
    pair = jnp.concatenate([own_projected, mixed], axis=1)
    share(2, jnp.where(my == 0, pair, pltpu.roll(pair, modes, 1)))

    step = 16
    row_id = lax.broadcasted_iota(jnp.int32, (modes, modes), 0)
    col_id = lax.broadcasted_iota(jnp.int32, (modes, modes), 1)
    small = lax.broadcasted_iota(jnp.int32, (step, 1), 0)
    lanes = lax.broadcasted_iota(jnp.int32, (step, width), 1)

    def exact(left, right, dims):
        return lax.dot_general(
            left, right, dims, precision=EXACT, preferred_element_type=jnp.float32
        )

    def factor_inverse(gram):
        eye = (row_id == col_id).astype(jnp.float32)
        work[...] = jnp.concatenate([gram, eye], axis=1)

        @pl.loop(0, modes // step)
        def _(b):
            begin = pl.multiple_of(b * step, step)
            panel = work[pl.ds(begin, step), :]
            near = panel
            columns = [
                jnp.sum(jnp.where(lanes == begin + s, near, 0.0), axis=1, keepdims=True)
                for s in range(step)
            ]
            pivots = jnp.zeros((step, 1), jnp.float32)
            for q in range(step):
                pivot = columns[q][q : q + 1, :]
                pivots = jnp.where(small == q, pivot, pivots)
                if q == step - 1:
                    break
                factor = jnp.where(small > q, columns[q] / pivot, 0.0)
                panel = panel - factor * panel[q : q + 1, :]
                for s in range(q + 1, step):
                    columns[s] = columns[s] - factor * columns[s][q : q + 1, :]
            inv_ref[pl.ds(begin, step), :] = panel / jnp.sqrt(pivots)
            ahead = (lanes >= begin + step) & (lanes < modes)
            below = jnp.where(ahead, panel / pivots, 0.0)[:, :modes]
            work[...] = work[...] - exact(below, panel, TN)

        return inv_ref[...][:, modes:]

    gram0, gram1 = arrived(0)
    gram0, gram1 = unfold(gram0), unfold(gram1)
    inv00 = factor_inverse(gram0)
    cross0, cross1 = arrived(1)
    bridge = exact(inv00, unfold(cross0 + cross1), NN)
    rest = gram1 - exact(bridge, bridge, TN)
    turn = exact(bridge, inv00, TN)
    total(2)
    inv11 = factor_inverse(rest)
    inv10 = -exact(inv11, turn, NN)
    lower = jnp.concatenate([inv10, inv11], axis=1)
    upper = jnp.concatenate([inv00, jnp.zeros((modes, modes), jnp.float32)], axis=1)
    inverse = jnp.concatenate([upper, lower], axis=0)
    own = jnp.where(my == 0, upper, pltpu.roll(lower, modes, 1))
    inv_t[...] = own.astype(jnp.bfloat16)
    for t in range(0, tiles, 2):
        two = jnp.concatenate(
            [jnp.concatenate([level2[u], other[u]], axis=0) for u in (t, t + 1)], axis=1
        )
        basis_ref[:, t * size : (t + 2) * size] = lax.dot_general(
            inv_t[...], two, NN, preferred_element_type=jnp.float32
        ).astype(jnp.bfloat16)
    projected0, projected1 = arrived(2)
    projected_t = jnp.concatenate([projected0, projected1], axis=0)
    ritz_ref[...] = exact(exact(inverse, projected_t, NT), inverse, NT)
    for c in range(chunks):
        exchange(c, my).wait_send()
    for k in range(3):
        sent(k)


def shards(parts, stiffness_tiles, tile_cols, send_rows, block, lower_bound, upper_bound):
    row_count, modes = block.shape
    tiles, nnz, size = stiffness_tiles.shape[:3]
    slots = send_rows.shape[1]
    width = 2 * modes
    assert parts >= 16 and parts % 2 == 0
    chunks = 5
    smem = pl.BlockSpec(memory_space=pltpu.SMEM)
    vmem = pl.BlockSpec(memory_space=pltpu.VMEM)
    hbm = pl.BlockSpec(memory_space=pl.ANY)
    dma = pltpu.SemaphoreType.DMA
    level = pltpu.VMEM((tiles + 2 * slots, modes, size), jnp.bfloat16)
    field = pltpu.VMEM((tiles, modes, size), jnp.bfloat16)
    basis, ritz = pl.pallas_call(
        functools.partial(kernel, parts),
        out_shape=(
            jax.ShapeDtypeStruct((modes, row_count), jnp.bfloat16),
            jax.ShapeDtypeStruct((width, width), jnp.float32),
        ),
        in_specs=[smem, smem, smem, smem, hbm, hbm],
        out_specs=(vmem, vmem),
        scratch_shapes=[
            pltpu.VMEM(stiffness_tiles.shape, jnp.bfloat16),
            pltpu.VMEM((tiles, nnz * size, size), jnp.bfloat16),
            level, level, level, pltpu.VMEM((modes, row_count), jnp.bfloat16), field, field, field,
            pltpu.VMEM((3, 2, slots, modes, size), jnp.bfloat16),
            pltpu.VMEM((3, 8, 8, width), jnp.float32),
            pltpu.VMEM((3 * parts, 8, width), jnp.float32),
            pltpu.VMEM((3, 16, 8, width), jnp.float32),
            pltpu.VMEM((3, 8, width), jnp.float32),
            pltpu.VMEM((modes, width), jnp.float32),
            pltpu.VMEM((modes, width), jnp.float32),
            pltpu.VMEM((modes, width), jnp.bfloat16),
            dma((1,)), dma((8,)), dma((3, 2)), dma((3, 2)), dma((chunks,)), dma((chunks,)),
            dma((3,)), dma((3,)), dma((3,)), dma((3,)),
        ],
        compiler_params=pltpu.CompilerParams(
            collective_id=0, has_side_effects=True, vmem_limit_bytes=60 * 1024 * 1024
        ),
    )(tile_cols.T, send_rows, lower_bound, upper_bound, block.T, stiffness_tiles)
    return basis.T, ritz


def solution(mesh):
    placed = (
        P("dof", None, None, None),
        P("dof", None),
        P("dof", None),
        P("dof", "mode"),
        P(),
        P(),
    )
    return jax.shard_map(
        functools.partial(shards, mesh.shape["dof"]),
        mesh=mesh, in_specs=placed, out_specs=(P("dof", "mode"), P()), check_vma=False,
    )
```

```python
import functools

import jax
import jax.numpy as jnp
from jax import lax
from jax.experimental import pallas as pl
from jax.experimental.pallas import tpu as pltpu
from jax.sharding import PartitionSpec as P

MESH = pl.DeviceIdType.MESH
GROUP = 16
NT = (((1,), (1,)), ((), ()))
NN = (((1,), (0,)), ((), ()))
TN = (((0,), (0,)), ((), ()))
EXACT = lax.Precision.HIGHEST


def kernel(
    parts, cols_hbm, rows_hbm, low_hbm, high_hbm, x_hbm, a_hbm, fields_ref, inv_t, ritz_ref,
    a_ref, turned, level0, level1, level2, x_ref, plain, image, other, sends,
    shares, gathered, totals, sums, work, inv_ref,
    cols, rows, low_ref, high_ref, x_sem, a_sem, keep_sem, halo_send, halo_recv, mode_send, mode_recv,
    share_send, share_recv, total_send, total_recv,
):
    tiles, nnz, size = a_ref.shape[0], a_ref.shape[1], a_ref.shape[2]
    modes = x_hbm.shape[0]
    width = 2 * modes
    slots = rows.shape[1]
    tables = [(cols_hbm, cols), (rows_hbm, rows), (low_hbm, low_ref), (high_hbm, high_ref)]
    tables = [pltpu.make_async_copy(*pair, x_sem.at[1 + i]) for i, pair in enumerate(tables)]
    chunks = mode_send.shape[0]
    p = lax.axis_index("dof")
    my = lax.axis_index("mode")
    has_low = p > 0
    has_up = p < parts - 1

    odd = lax.rem(p, 2)
    mate = p + 1 - 2 * odd
    far = p - 1 + 2 * odd
    has_far = (far >= 0) & (far < parts)
    far_slot = lax.rem(far + parts, parts)

    fetch = pltpu.make_async_copy(x_hbm, x_ref, x_sem.at[0])
    fetch.start()
    for table in tables:
        table.start()
    barrier = pltpu.get_barrier_semaphore()

    @pl.loop(1, 2 * parts)
    def _(d):
        peer = (lax.rem(p + d // 2, parts), lax.rem(my + d, 2))
        pl.semaphore_signal(barrier, inc=1, device_id=peer, device_id_type=MESH)

    fetch.wait()
    loads = []
    a_parts = a_sem.shape[0]
    share = tiles // a_parts
    for i in range(a_parts):
        span = pl.ds(i * share, share)
        loads.append(pltpu.make_async_copy(a_hbm.at[span], a_ref.at[span], a_sem.at[i]))
        loads[-1].start()
    for table in tables:
        table.wait()

    for t in range(tiles):
        plain[t] = x_ref[:, t * size : (t + 1) * size]
    for s in range(slots):
        for which, row in enumerate((rows[odd, s], rows[1 - odd, s])):
            sends[0, which, s] = plain[row]

    @pl.when(p == 0)
    def _():
        for level in (level0, level1, level2):
            level[tiles : tiles + slots] = jnp.zeros((slots, modes, size), jnp.bfloat16)

    @pl.when(p == parts - 1)
    def _():
        for level in (level0, level1, level2):
            level[tiles + slots :] = jnp.zeros((slots, modes, size), jnp.bfloat16)

    pl.semaphore_wait(barrier, 2 * parts - 1)

    def halo(index, level, remote):
        hop = odd if remote else 1 - odd
        return pltpu.make_async_remote_copy(
            src_ref=sends.at[index, 0 if remote else 1],
            dst_ref=level.at[pl.ds(tiles + slots * (1 - hop), slots)],
            send_sem=halo_send.at[index, 0 if remote else 1],
            recv_sem=halo_recv.at[index, 0 if remote else 1],
            device_id=(far_slot if remote else mate, my),
            device_id_type=MESH,
        )

    def start_far(index, level):
        pl.when(has_far)(halo(index, level, True).start)

    def start_near(index, level):
        halo(index, level, False).start()

    def wait_halo(index, level):
        near, remote = halo(index, level, False), halo(index, level, True)
        near.wait_recv()
        near.wait_send()
        pl.when(has_far)(remote.wait_recv)
        pl.when(has_far)(remote.wait_send)

    start_far(0, level0)
    start_near(0, level0)
    for t in range(tiles):
        level0[t] = plain[t]

    center = (high_ref[0] + low_ref[0]) * 0.5
    half_width = (high_ref[0] - low_ref[0]) * 0.5
    scale = jnp.ones((1, size), jnp.float32) / jnp.full((1, size), half_width, jnp.float32)

    def product(level, t):
        field = jnp.concatenate([level[cols[k, t]] for k in range(nnz)], axis=1)
        return lax.dot_general(field, turned[t], NN, preferred_element_type=jnp.float32)

    def first(t):
        own = level0[t].astype(jnp.float32)
        return ((product(level0, t) - center * own) * scale).astype(jnp.bfloat16)

    def second(t):
        own = level1[t].astype(jnp.float32)
        before = level0[t].astype(jnp.float32)
        return (2.0 * (product(level1, t) - center * own) * scale - before).astype(jnp.bfloat16)

    def send_tiles(index, which, make):
        made = [make(rows[odd if which == 0 else 1 - odd, s]) for s in range(slots)]
        for s, value in enumerate(made):
            sends[index, which, s] = value

    def all_tiles(make, target, begin, count, group=GROUP):
        group = min(group, count)

        @pl.loop(0, count // group)
        def _(i):
            made = [make(begin + i * group + u) for u in range(group)]
            for u in range(group):
                target[begin + i * group + u] = made[u]

    for i, load in enumerate(loads):
        load.wait()

        @pl.loop(0, share // 2)
        def _(j):
            for u in range(2):
                t = i * share + j * 2 + u
                for k in range(nnz):
                    turned[t, k * size : (k + 1) * size] = a_ref[t, k].T

    wait_halo(0, level0)
    send_tiles(1, 0, first)
    start_far(1, level1)
    send_tiles(1, 1, first)
    start_near(1, level1)
    all_tiles(first, level1, 0, tiles)
    wait_halo(1, level1)
    half = tiles // 2
    quarter = half // 4
    pieces = [(0, quarter), (quarter, quarter), (2 * quarter, 2 * quarter)]
    pieces = [(0, *piece) for piece in pieces] + [(1, 0, half // 2), (1, half // 2, half // 2)]
    urgent = range(3)
    later = range(3, 5)

    def exchange(c, sender):
        which, offset, count = pieces[c]
        begin = (sender if which == 0 else 1 - sender) * half + offset
        span = pl.ds(begin, count)
        return pltpu.make_async_remote_copy(
            src_ref=level2.at[span],
            dst_ref=other.at[span],
            send_sem=mode_send.at[c],
            recv_sem=mode_recv.at[c],
            device_id=(p, 1 - my),
            device_id_type=MESH,
        )

    def exchanged(c):
        which, offset, count = pieces[c]
        begin = (my if which == 0 else 1 - my) * half + offset
        all_tiles(second, level2, begin, count)
        exchange(c, my).start()

    block = shares.shape[2]
    base = (parts - 8) // 2

    def owners(k):
        return [base + k + 2 * b for b in range(4)] if k < 2 else [base + b for b in range(8)]

    def owned(k):
        place = p - base
        inside = (place >= 0) & (place < 8)
        return inside & (lax.rem(place + 8, 2) == k) if k < 2 else inside

    def blocks_wait(ref, count, sem):
        view = ref.at[pl.ds(0, count)]
        pltpu.make_async_copy(view, view, sem).wait()

    def share(k, value):
        for b, owner in enumerate(owners(k)):
            shares[k, b] = value[b * block : (b + 1) * block]
        for b, owner in enumerate(owners(k)):
            copy = pltpu.make_async_remote_copy(
                src_ref=shares.at[k, b],
                dst_ref=gathered.at[k * parts + p],
                send_sem=share_send.at[k],
                recv_sem=share_recv.at[k],
                device_id=(owner, my),
                device_id_type=MESH,
            )
            pl.when(p != owner)(copy.start)

            @pl.when(p == owner)
            def _():
                gathered[k * parts + p] = shares[k, b]

    def total(k):
        count = len(owners(k))

        @pl.when(owned(k))
        def _():
            blocks_wait(gathered, parts - 1, share_recv.at[k])
            value = gathered[k * parts]
            for q in range(1, parts):
                value = value + gathered[k * parts + q]
            sums[k] = value
            slot = my * count + (p - base) // (8 // count)
            totals[k, slot] = value

            @pl.loop(1, 2 * parts)
            def _(d):
                pltpu.make_async_remote_copy(
                    src_ref=sums.at[k],
                    dst_ref=totals.at[k, slot],
                    send_sem=total_send.at[k],
                    recv_sem=total_recv.at[k],
                    device_id=(lax.rem(p + d // 2, parts), lax.rem(my + d, 2)),
                    device_id_type=MESH,
                ).start()

    def arrived(k):
        count = len(owners(k))

        @pl.when(owned(k))
        def _():
            blocks_wait(totals.at[k], 2 * count - 1, total_recv.at[k])

        @pl.when(jnp.logical_not(owned(k)))
        def _():
            blocks_wait(totals.at[k], 2 * count, total_recv.at[k])

        flat = totals[k, : 2 * count].reshape(2, count * block, width) / (parts * tiles * size)
        return flat[0], flat[1]

    def sent(k):
        count = len(owners(k))

        @pl.when(owned(k))
        def _():
            blocks_wait(shares.at[k], count - 1, share_send.at[k])
            blocks_wait(gathered, 2 * parts - 1, total_send.at[k])

        @pl.when(jnp.logical_not(owned(k)))
        def _():
            blocks_wait(shares.at[k], count, share_send.at[k])

    def contract(left, right, begin, count):
        acc = jnp.zeros((modes, modes), jnp.float32)
        for i in range(0, count, 8):
            lhs = jnp.concatenate([left[begin + i + u] for u in range(8)], axis=1)
            rhs = jnp.concatenate([right[begin + i + u] for u in range(8)], axis=1)
            acc = acc + lax.dot_general(lhs, rhs, NT, preferred_element_type=jnp.float32)
        return acc

    def fold(value):
        return jnp.concatenate([value[: modes // 2], value[modes // 2 :]], axis=1)

    def unfold(value):
        return jnp.concatenate([value[:, :modes], value[:, modes:]], axis=0)

    for c in urgent:
        exchanged(c)
    send_tiles(2, 0, second)
    start_far(2, level2)
    send_tiles(2, 1, second)
    start_near(2, level2)
    for c in later:
        exchanged(c)
    keep_own = pltpu.make_async_copy(level2.at[pl.ds(0, tiles)], fields_ref.at[0], keep_sem.at[0])
    keep_own.start()
    share(0, fold(contract(level2, level2, 0, tiles)))
    wait_halo(2, level2)
    all_tiles(lambda t: product(level2, t).astype(jnp.bfloat16), image, 0, tiles)
    for c in urgent:
        exchange(c, 1 - my).wait_recv()
    cross = contract(level2, other, (1 - my) * half, half)
    share(1, fold(jnp.where(my == 0, cross, cross.T)))
    total(0)
    own_projected = contract(image, level2, 0, tiles)
    mixed = contract(image, other, (1 - my) * half, half)
    total(1)
    for c in later:
        exchange(c, 1 - my).wait_recv()
    keep_other = pltpu.make_async_copy(other, fields_ref.at[1], keep_sem.at[1])
    keep_other.start()
    mixed = mixed + contract(image, other, my * half, half)
    pair = jnp.concatenate([own_projected, mixed], axis=1)
    share(2, jnp.where(my == 0, pair, pltpu.roll(pair, modes, 1)))

    step = 16
    row_id = lax.broadcasted_iota(jnp.int32, (modes, modes), 0)
    col_id = lax.broadcasted_iota(jnp.int32, (modes, modes), 1)
    small = lax.broadcasted_iota(jnp.int32, (step, 1), 0)
    lanes = lax.broadcasted_iota(jnp.int32, (step, width), 1)

    def exact(left, right, dims):
        return lax.dot_general(
            left, right, dims, precision=EXACT, preferred_element_type=jnp.float32
        )

    def factor_inverse(gram):
        eye = (row_id == col_id).astype(jnp.float32)
        work[...] = jnp.concatenate([gram, eye], axis=1)

        @pl.loop(0, modes // step)
        def _(b):
            begin = pl.multiple_of(b * step, step)
            panel = work[pl.ds(begin, step), :]
            near = panel
            columns = [
                jnp.sum(jnp.where(lanes == begin + s, near, 0.0), axis=1, keepdims=True)
                for s in range(step)
            ]
            pivots = jnp.zeros((step, 1), jnp.float32)
            for q in range(step):
                pivot = columns[q][q : q + 1, :]
                pivots = jnp.where(small == q, pivot, pivots)
                if q == step - 1:
                    break
                factor = jnp.where(small > q, columns[q] / pivot, 0.0)
                panel = panel - factor * panel[q : q + 1, :]
                for s in range(q + 1, step):
                    columns[s] = columns[s] - factor * columns[s][q : q + 1, :]
            inv_ref[pl.ds(begin, step), :] = panel / jnp.sqrt(pivots)
            ahead = (lanes >= begin + step) & (lanes < modes)
            below = jnp.where(ahead, panel / pivots, 0.0)[:, :modes]
            work[...] = work[...] - exact(below, panel, TN)

        return inv_ref[...][:, modes:]

    gram0, gram1 = arrived(0)
    gram0, gram1 = unfold(gram0), unfold(gram1)
    inv00 = factor_inverse(gram0)
    cross0, cross1 = arrived(1)
    bridge = exact(inv00, unfold(cross0 + cross1), NN)
    rest = gram1 - exact(bridge, bridge, TN)
    turn = exact(bridge, inv00, TN)
    total(2)
    inv11 = factor_inverse(rest)
    inv10 = -exact(inv11, turn, NN)
    lower = jnp.concatenate([inv10, inv11], axis=1)
    upper = jnp.concatenate([inv00, jnp.zeros((modes, modes), jnp.float32)], axis=1)
    inverse = jnp.concatenate([upper, lower], axis=0)
    own = jnp.where(my == 0, upper, pltpu.roll(lower, modes, 1))
    inv_t[...] = own.astype(jnp.bfloat16)
    projected0, projected1 = arrived(2)
    projected_t = jnp.concatenate([projected0, projected1], axis=0)
    ritz_ref[...] = exact(exact(inverse, projected_t, NT), inverse, NT)
    keep_own.wait()
    keep_other.wait()
    for c in range(chunks):
        exchange(c, my).wait_send()
    for k in range(3):
        sent(k)


def finish(fields, inv_t, ritz_in, basis_ref, ritz_ref):
    tiles, size = fields.shape[1], fields.shape[3]
    ritz_ref[...] = ritz_in[...]
    for t in range(0, tiles, 2):
        pair = jnp.concatenate(
            [jnp.concatenate([fields[0, u], fields[1, u]], axis=0) for u in (t, t + 1)], axis=1
        )
        basis_ref[:, t * size : (t + 2) * size] = lax.dot_general(
            inv_t[...], pair, NN, preferred_element_type=jnp.float32
        ).astype(jnp.bfloat16)


def shards(parts, stiffness_tiles, tile_cols, send_rows, block, lower_bound, upper_bound):
    row_count, modes = block.shape
    tiles, nnz, size = stiffness_tiles.shape[:3]
    slots = send_rows.shape[1]
    width = 2 * modes
    assert parts >= 16 and parts % 2 == 0
    chunks = 5
    vmem = pl.BlockSpec(memory_space=pltpu.VMEM)
    hbm = pl.BlockSpec(memory_space=pl.ANY)
    far = pl.BlockSpec(memory_space=pltpu.HBM)
    dma = pltpu.SemaphoreType.DMA
    level = pltpu.VMEM((tiles + 2 * slots, modes, size), jnp.bfloat16)
    field = pltpu.VMEM((tiles, modes, size), jnp.bfloat16)
    fields, inv_t, ritz = pl.pallas_call(
        functools.partial(kernel, parts),
        out_shape=(
            jax.ShapeDtypeStruct((2, tiles, modes, size), jnp.bfloat16),
            jax.ShapeDtypeStruct((modes, width), jnp.bfloat16),
            jax.ShapeDtypeStruct((width, width), jnp.float32),
        ),
        in_specs=[far] * 6,
        out_specs=(hbm, vmem, vmem),
        scratch_shapes=[
            pltpu.VMEM(stiffness_tiles.shape, jnp.bfloat16),
            pltpu.VMEM((tiles, nnz * size, size), jnp.bfloat16),
            level, level, level, pltpu.VMEM((modes, row_count), jnp.bfloat16), field, field, field,
            pltpu.VMEM((3, 2, slots, modes, size), jnp.bfloat16),
            pltpu.VMEM((3, 8, 8, width), jnp.float32),
            pltpu.VMEM((3 * parts, 8, width), jnp.float32),
            pltpu.VMEM((3, 16, 8, width), jnp.float32),
            pltpu.VMEM((3, 8, width), jnp.float32),
            pltpu.VMEM((modes, width), jnp.float32),
            pltpu.VMEM((modes, width), jnp.float32),
            pltpu.SMEM((nnz, tiles), jnp.int32),
            pltpu.SMEM(send_rows.shape, jnp.int32),
            pltpu.SMEM((1,), jnp.float32),
            pltpu.SMEM((1,), jnp.float32),
            dma((5,)), dma((8,)), dma((2,)), dma((3, 2)), dma((3, 2)), dma((chunks,)), dma((chunks,)),
            dma((3,)), dma((3,)), dma((3,)), dma((3,)),
        ],
        compiler_params=pltpu.CompilerParams(
            collective_id=0, has_side_effects=True, vmem_limit_bytes=50331648
        ),
    )(
        *[pltpu.with_memory_space_constraint(ref, pltpu.HBM) for ref in (tile_cols.T, send_rows)],
        lower_bound, upper_bound,
        *[pltpu.with_memory_space_constraint(ref, pltpu.HBM) for ref in (block.T, stiffness_tiles)],
    )
    basis, ritz = pl.pallas_call(
        finish,
        out_shape=(
            jax.ShapeDtypeStruct((modes, row_count), jnp.bfloat16),
            jax.ShapeDtypeStruct((width, width), jnp.float32),
        ),
        in_specs=[vmem, vmem, vmem],
        out_specs=(vmem, vmem),
        compiler_params=pltpu.CompilerParams(vmem_limit_bytes=8 * 1024 * 1024),
    )(fields, inv_t, ritz)
    return basis.T, ritz


def solution(mesh):
    placed = (
        P("dof", None, None, None),
        P("dof", None),
        P("dof", None),
        P("dof", "mode"),
        P(),
        P(),
    )
    return jax.shard_map(
        functools.partial(shards, mesh.shape["dof"]),
        mesh=mesh, in_specs=placed, out_specs=(P("dof", "mode"), P()), check_vma=False,
    )
```

```python
import functools

import jax
import jax.numpy as jnp
from jax import lax
from jax.experimental import pallas as pl
from jax.experimental.pallas import tpu as pltpu
from jax.sharding import PartitionSpec as P

MESH = pl.DeviceIdType.MESH
GROUP = 16
NT = (((1,), (1,)), ((), ()))
NN = (((1,), (0,)), ((), ()))
TN = (((0,), (0,)), ((), ()))
EXACT = lax.Precision.HIGHEST


def kernel(
    parts, cols_hbm, rows_hbm, low_hbm, high_hbm, x_hbm, a_hbm, basis_ref, ritz_ref,
    a_ref, turned, level0, level1, level2, x_ref, plain, image, other, sends,
    shares, gathered, totals, sums, work, inv_ref, inv_t, basis,
    cols, rows, low_ref, high_ref, x_sem, a_sem, keep_sem, halo_send, halo_recv, mode_send, mode_recv,
    share_send, share_recv, total_send, total_recv,
):
    tiles, nnz, size = a_ref.shape[0], a_ref.shape[1], a_ref.shape[2]
    modes = x_hbm.shape[0]
    width = 2 * modes
    slots = rows.shape[1]
    tables = [(cols_hbm, cols), (rows_hbm, rows), (low_hbm, low_ref), (high_hbm, high_ref)]
    tables = [pltpu.make_async_copy(*pair, x_sem.at[1 + i]) for i, pair in enumerate(tables)]
    chunks = mode_send.shape[0]
    p = lax.axis_index("dof")
    my = lax.axis_index("mode")
    has_low = p > 0
    has_up = p < parts - 1

    odd = lax.rem(p, 2)
    mate = p + 1 - 2 * odd
    far = p - 1 + 2 * odd
    has_far = (far >= 0) & (far < parts)
    far_slot = lax.rem(far + parts, parts)

    fetch = pltpu.make_async_copy(x_hbm, x_ref, x_sem.at[0])
    fetch.start()
    for table in tables:
        table.start()
    loads = []
    a_parts = a_sem.shape[0]
    span = tiles // a_parts
    for i in range(a_parts):
        view = pl.ds(i * span, span)
        loads.append(pltpu.make_async_copy(a_hbm.at[view], a_ref.at[view], a_sem.at[i]))
    for load in loads[:2]:
        load.start()

    def peer(shift, other_mode):
        place = p + shift
        place = jnp.where(place >= parts, place - parts, place)
        return place, 1 - my if other_mode else my

    near_first = sorted(
        ((d, e) for d in range(parts) for e in range(2) if d or e),
        key=lambda pair: (min(pair[0], parts - pair[0]), pair[1]),
    )
    barrier = pltpu.get_barrier_semaphore()
    for shift, other_mode in near_first:
        pl.semaphore_signal(
            barrier, inc=1, device_id=peer(shift, other_mode), device_id_type=MESH
        )
    fetch.wait()
    for load in loads[2:]:
        load.start()
    for table in tables:
        table.wait()

    for t in range(tiles):
        plain[t] = x_ref[:, t * size : (t + 1) * size]
    for s in range(slots):
        for which, row in enumerate((rows[odd, s], rows[1 - odd, s])):
            sends[0, which, s] = plain[row]

    @pl.when(p == 0)
    def _():
        for level in (level0, level1, level2):
            level[tiles : tiles + slots] = jnp.zeros((slots, modes, size), jnp.bfloat16)

    @pl.when(p == parts - 1)
    def _():
        for level in (level0, level1, level2):
            level[tiles + slots :] = jnp.zeros((slots, modes, size), jnp.bfloat16)

    pl.semaphore_wait(barrier, 2 * parts - 1)

    def halo(index, level, which):
        hop = 1 - odd if which == 2 else odd
        count = slots if which == 2 else slots // 2
        first_slot = slots // 2 if which == 1 else 0
        return pltpu.make_async_remote_copy(
            src_ref=sends.at[index, which // 2, pl.ds(first_slot, count)],
            dst_ref=level.at[pl.ds(tiles + slots * (1 - hop) + first_slot, count)],
            send_sem=halo_send.at[index, which],
            recv_sem=halo_recv.at[index, which],
            device_id=(mate if which == 2 else far_slot, my),
            device_id_type=MESH,
        )

    def start_far(index, level, which):
        pl.when(has_far)(halo(index, level, which).start)

    def start_near(index, level):
        halo(index, level, 2).start()

    def wait_halo(index, level):
        near = halo(index, level, 2)
        near.wait_recv()
        near.wait_send()
        for which in range(2):
            copy = halo(index, level, which)
            pl.when(has_far)(copy.wait_recv)
            pl.when(has_far)(copy.wait_send)

    start_far(0, level0, 0)
    start_far(0, level0, 1)
    start_near(0, level0)
    for t in range(tiles):
        level0[t] = plain[t]

    center = (high_ref[0] + low_ref[0]) * 0.5
    half_width = (high_ref[0] - low_ref[0]) * 0.5
    scale = jnp.ones((1, size), jnp.float32) / jnp.full((1, size), half_width, jnp.float32)

    def product(level, t):
        field = jnp.concatenate([level[cols[k, t]] for k in range(nnz)], axis=1)
        return lax.dot_general(field, turned[t], NN, preferred_element_type=jnp.float32)

    def first(t):
        own = level0[t].astype(jnp.float32)
        return ((product(level0, t) - center * own) * scale).astype(jnp.bfloat16)

    def second(t):
        own = level1[t].astype(jnp.float32)
        before = level0[t].astype(jnp.float32)
        return (2.0 * (product(level1, t) - center * own) * scale - before).astype(jnp.bfloat16)

    def send_tiles(index, level, make):
        for which in range(2):
            begin = which * (slots // 2)
            made = [make(rows[odd, begin + u]) for u in range(slots // 2)]
            for u, value in enumerate(made):
                sends[index, 0, begin + u] = value
            start_far(index, level, which)
        made = [make(rows[1 - odd, u]) for u in range(slots)]
        for u, value in enumerate(made):
            sends[index, 1, u] = value
        start_near(index, level)

    def all_tiles(make, target, begin, count, group=GROUP):
        group = min(group, count)

        @pl.loop(0, count // group)
        def _(i):
            made = [make(begin + i * group + u) for u in range(group)]
            for u in range(group):
                target[begin + i * group + u] = made[u]

    for i, load in enumerate(loads):
        load.wait()

        @pl.loop(0, span // 2)
        def _(j):
            for u in range(2):
                t = i * span + j * 2 + u
                for k in range(nnz):
                    turned[t, k * size : (k + 1) * size] = a_ref[t, k].T

    wait_halo(0, level0)
    send_tiles(1, level1, first)
    all_tiles(first, level1, 0, tiles)
    wait_halo(1, level1)
    half = tiles // 2
    quarter = half // 4
    pieces = [(0, quarter), (quarter, quarter), (2 * quarter, 2 * quarter)]
    pieces = [(0, *piece) for piece in pieces] + [(1, 0, half // 2), (1, half // 2, half // 2)]
    urgent = range(3)
    later = range(3, 5)

    def exchange(c, sender):
        which, offset, count = pieces[c]
        begin = (sender if which == 0 else 1 - sender) * half + offset
        span = pl.ds(begin, count)
        return pltpu.make_async_remote_copy(
            src_ref=level2.at[span],
            dst_ref=other.at[span],
            send_sem=mode_send.at[c],
            recv_sem=mode_recv.at[c],
            device_id=(p, 1 - my),
            device_id_type=MESH,
        )

    def exchanged(c):
        which, offset, count = pieces[c]
        begin = (my if which == 0 else 1 - my) * half + offset
        all_tiles(second, level2, begin, count)
        exchange(c, my).start()

    block = shares.shape[2]
    base = (parts - 8) // 2

    def owners(k):
        return [base + b for b in range(8)] if k == 2 else [base + k % 2 + 2 * b for b in range(4)]

    def owned(k):
        place = p - base
        inside = (place >= 0) & (place < 8)
        return inside if k == 2 else inside & (lax.rem(p - base + parts, 2) == k % 2)

    def blocks_wait(ref, count, sem):
        view = ref.at[pl.ds(0, count)]
        pltpu.make_async_copy(view, view, sem).wait()

    def share(k, value):
        for b, owner in enumerate(owners(k)):
            shares[k, b] = value[b * block : (b + 1) * block]
        for b, owner in enumerate(owners(k)):
            copy = pltpu.make_async_remote_copy(
                src_ref=shares.at[k, b],
                dst_ref=gathered.at[k * parts + p],
                send_sem=share_send.at[k],
                recv_sem=share_recv.at[k],
                device_id=(owner, my),
                device_id_type=MESH,
            )
            pl.when(p != owner)(copy.start)

            @pl.when(p == owner)
            def _():
                gathered[k * parts + p] = shares[k, b]

    def total(k):
        count = len(owners(k))

        @pl.when(owned(k))
        def _():
            blocks_wait(gathered, parts - 1, share_recv.at[k])
            value = gathered[k * parts]
            for q in range(1, parts):
                value = value + gathered[k * parts + q]
            sums[k] = value
            slot = my * count + (p - base) // (8 // count)
            totals[k, slot] = value

            for shift, other_mode in reversed(near_first):
                pltpu.make_async_remote_copy(
                    src_ref=sums.at[k],
                    dst_ref=totals.at[k, slot],
                    send_sem=total_send.at[k],
                    recv_sem=total_recv.at[k],
                    device_id=peer(shift, other_mode),
                    device_id_type=MESH,
                ).start()

    def arrived(k):
        count = len(owners(k))

        @pl.when(owned(k))
        def _():
            blocks_wait(totals.at[k], 2 * count - 1, total_recv.at[k])

        @pl.when(jnp.logical_not(owned(k)))
        def _():
            blocks_wait(totals.at[k], 2 * count, total_recv.at[k])

        flat = totals[k, : 2 * count].reshape(2, count * block, width) / (parts * tiles * size)
        return flat[0], flat[1]

    def sent(k):
        count = len(owners(k))

        @pl.when(owned(k))
        def _():
            blocks_wait(shares.at[k], count - 1, share_send.at[k])
            blocks_wait(gathered, 2 * parts - 1, total_send.at[k])

        @pl.when(jnp.logical_not(owned(k)))
        def _():
            blocks_wait(shares.at[k], count, share_send.at[k])

    def contract(left, right, begin, count):
        acc = jnp.zeros((modes, modes), jnp.float32)
        for i in range(0, count, 8):
            lhs = jnp.concatenate([left[begin + i + u] for u in range(8)], axis=1)
            rhs = jnp.concatenate([right[begin + i + u] for u in range(8)], axis=1)
            acc = acc + lax.dot_general(lhs, rhs, NT, preferred_element_type=jnp.float32)
        return acc

    def fold(value):
        return jnp.concatenate([value[: modes // 2], value[modes // 2 :]], axis=1)

    def unfold(value):
        return jnp.concatenate([value[:, :modes], value[:, modes:]], axis=0)

    for c in urgent:
        exchanged(c)
    send_tiles(2, level2, second)
    for c in later:
        exchanged(c)
    share(0, fold(contract(level2, level2, 0, tiles)))
    wait_halo(2, level2)
    all_tiles(lambda t: product(level2, t).astype(jnp.bfloat16), image, 0, tiles)
    for c in urgent:
        exchange(c, 1 - my).wait_recv()
    cross = contract(level2, other, (1 - my) * half, half)
    share(1, fold(jnp.where(my == 0, cross, cross.T)))
    total(0)
    own_projected = contract(image, level2, 0, tiles)
    mixed = contract(image, other, (1 - my) * half, half)
    pair = jnp.concatenate([own_projected, mixed], axis=1)
    share(2, jnp.where(my == 0, pair, pltpu.roll(pair, modes, 1)))
    total(1)
    total(2)
    rest_begin = my * half
    exchange(3, 1 - my).wait_recv()
    mixed = contract(image, other, rest_begin, half // 2)
    exchange(4, 1 - my).wait_recv()
    share(3, fold(mixed + contract(image, other, rest_begin + half // 2, half // 2)))

    step = 16
    row_id = lax.broadcasted_iota(jnp.int32, (modes, modes), 0)
    col_id = lax.broadcasted_iota(jnp.int32, (modes, modes), 1)
    small = lax.broadcasted_iota(jnp.int32, (step, 1), 0)
    lanes = lax.broadcasted_iota(jnp.int32, (step, width), 1)

    def exact(left, right, dims):
        return lax.dot_general(
            left, right, dims, precision=EXACT, preferred_element_type=jnp.float32
        )

    def factor_inverse(gram):
        eye = (row_id == col_id).astype(jnp.float32)
        work[...] = jnp.concatenate([gram, eye], axis=1)

        @pl.loop(0, modes // step)
        def _(b):
            begin = pl.multiple_of(b * step, step)
            panel = work[pl.ds(begin, step), :]
            near = panel
            columns = [
                jnp.sum(jnp.where(lanes == begin + s, near, 0.0), axis=1, keepdims=True)
                for s in range(step)
            ]
            pivots = jnp.zeros((step, 1), jnp.float32)
            for q in range(step):
                pivot = columns[q][q : q + 1, :]
                pivots = jnp.where(small == q, pivot, pivots)
                if q == step - 1:
                    break
                factor = jnp.where(small > q, columns[q] / pivot, 0.0)
                panel = panel - factor * panel[q : q + 1, :]
                for s in range(q + 1, step):
                    columns[s] = columns[s] - factor * columns[s][q : q + 1, :]
            inv_ref[pl.ds(begin, step), :] = panel / jnp.sqrt(pivots)
            ahead = (lanes >= begin + step) & (lanes < modes)
            below = jnp.where(ahead, panel / pivots, 0.0)[:, :modes]
            work[...] = work[...] - exact(below, panel, TN)

        return inv_ref[...][:, modes:]

    gram0, gram1 = arrived(0)
    gram0, gram1 = unfold(gram0), unfold(gram1)
    inv00 = factor_inverse(gram0)
    cross0, cross1 = arrived(1)
    bridge = exact(inv00, unfold(cross0 + cross1), NN)
    rest = gram1 - exact(bridge, bridge, TN)
    turn = exact(bridge, inv00, TN)
    total(3)
    inv11 = factor_inverse(rest)
    inv10 = -exact(inv11, turn, NN)
    lower = jnp.concatenate([inv10, inv11], axis=1)
    blank = jnp.zeros((modes, modes), jnp.float32)
    upper = jnp.concatenate([inv00, blank], axis=1)
    inverse = jnp.concatenate([upper, lower], axis=0)
    own = jnp.where(my == 0, upper, pltpu.roll(lower, modes, 1))
    inv_t[...] = own.astype(jnp.bfloat16)
    for t in range(0, tiles, 2):
        two = jnp.concatenate(
            [jnp.concatenate([level2[u], other[u]], axis=0) for u in (t, t + 1)], axis=1
        )
        basis[:, t * size : (t + 2) * size] = lax.dot_general(
            inv_t[...], two, NN, preferred_element_type=jnp.float32
        ).astype(jnp.bfloat16)
    keep = pltpu.make_async_copy(basis, basis_ref, keep_sem.at[0])
    keep.start()
    projected_t = jnp.concatenate(arrived(2), axis=0)
    late0, late1 = arrived(3)
    projected_t = projected_t + jnp.concatenate(
        [
            jnp.concatenate([blank, unfold(late0)], axis=1),
            jnp.concatenate([unfold(late1), blank], axis=1),
        ],
        axis=0,
    )
    ritz_ref[...] = exact(exact(inverse, projected_t, NT), inverse, NT)
    keep.wait()
    for c in range(chunks):
        exchange(c, my).wait_send()
    for k in range(4):
        sent(k)


def finish(basis_in, ritz_in, basis_ref, ritz_ref, sem):
    copies = [
        pltpu.make_async_copy(basis_in, basis_ref, sem.at[0]),
        pltpu.make_async_copy(ritz_in, ritz_ref, sem.at[1]),
    ]
    for copy in copies:
        copy.start()
    for copy in copies:
        copy.wait()


def shards(parts, stiffness_tiles, tile_cols, send_rows, block, lower_bound, upper_bound):
    row_count, modes = block.shape
    tiles, nnz, size = stiffness_tiles.shape[:3]
    slots = send_rows.shape[1]
    width = 2 * modes
    assert parts >= 16 and parts % 2 == 0
    chunks = 5
    vmem = pl.BlockSpec(memory_space=pltpu.VMEM)
    hbm = pl.BlockSpec(memory_space=pl.ANY)
    far = pl.BlockSpec(memory_space=pltpu.HBM)
    dma = pltpu.SemaphoreType.DMA
    level = pltpu.VMEM((tiles + 2 * slots, modes, size), jnp.bfloat16)
    field = pltpu.VMEM((tiles, modes, size), jnp.bfloat16)
    basis, ritz = pl.pallas_call(
        functools.partial(kernel, parts),
        out_shape=(
            jax.ShapeDtypeStruct((modes, row_count), jnp.bfloat16),
            jax.ShapeDtypeStruct((width, width), jnp.float32),
        ),
        in_specs=[far] * 6,
        out_specs=(hbm, vmem),
        scratch_shapes=[
            pltpu.VMEM(stiffness_tiles.shape, jnp.bfloat16),
            pltpu.VMEM((tiles, nnz * size, size), jnp.bfloat16),
            level, level, level, pltpu.VMEM((modes, row_count), jnp.bfloat16), field, field, field,
            pltpu.VMEM((3, 2, slots, modes, size), jnp.bfloat16),
            pltpu.VMEM((4, 8, 8, width), jnp.float32),
            pltpu.VMEM((4 * parts, 8, width), jnp.float32),
            pltpu.VMEM((4, 16, 8, width), jnp.float32),
            pltpu.VMEM((4, 8, width), jnp.float32),
            pltpu.VMEM((modes, width), jnp.float32),
            pltpu.VMEM((modes, width), jnp.float32),
            pltpu.VMEM((modes, width), jnp.bfloat16),
            pltpu.VMEM((modes, row_count), jnp.bfloat16),
            pltpu.SMEM((nnz, tiles), jnp.int32),
            pltpu.SMEM(send_rows.shape, jnp.int32),
            pltpu.SMEM((1,), jnp.float32),
            pltpu.SMEM((1,), jnp.float32),
            dma((5,)), dma((8,)), dma((1,)), dma((3, 3)), dma((3, 3)), dma((chunks,)), dma((chunks,)),
            dma((4,)), dma((4,)), dma((4,)), dma((4,)),
        ],
        compiler_params=pltpu.CompilerParams(
            collective_id=0, has_side_effects=True, vmem_limit_bytes=50331648
        ),
    )(
        *[pltpu.with_memory_space_constraint(ref, pltpu.HBM) for ref in (tile_cols.T, send_rows)],
        lower_bound, upper_bound,
        *[pltpu.with_memory_space_constraint(ref, pltpu.HBM) for ref in (block.T, stiffness_tiles)],
    )
    basis, ritz = pl.pallas_call(
        finish,
        out_shape=(
            jax.ShapeDtypeStruct((modes, row_count), jnp.bfloat16),
            jax.ShapeDtypeStruct((width, width), jnp.float32),
        ),
        in_specs=[hbm, hbm],
        out_specs=(hbm, hbm),
        scratch_shapes=[dma((2,))],
        compiler_params=pltpu.CompilerParams(vmem_limit_bytes=8 * 1024 * 1024),
    )(basis, ritz)
    return basis.T, ritz


def solution(mesh):
    placed = (
        P("dof", None, None, None),
        P("dof", None),
        P("dof", None),
        P("dof", "mode"),
        P(),
        P(),
    )
    return jax.shard_map(
        functools.partial(shards, mesh.shape["dof"]),
        mesh=mesh, in_specs=placed, out_specs=(P("dof", "mode"), P()), check_vma=False,
    )
```

```python
import functools

import jax
import jax.numpy as jnp
from jax import lax
from jax.experimental import pallas as pl
from jax.experimental.pallas import tpu as pltpu
from jax.sharding import PartitionSpec as P

MESH = pl.DeviceIdType.MESH
GROUP = 16
NT = (((1,), (1,)), ((), ()))
NN = (((1,), (0,)), ((), ()))
TN = (((0,), (0,)), ((), ()))
EXACT = lax.Precision.HIGHEST


def kernel(
    parts, cols_hbm, rows_hbm, low_hbm, high_hbm, x_hbm, a_hbm, basis_ref, ritz_ref,
    a_ref, turned, level0, level1, level2, x_ref, plain, image, other, sends,
    shares, gathered, totals, sums, work, inv_ref, inv_t, basis,
    cols, rows, low_ref, high_ref, spread_sem, x_sem, a_sem, keep_sem, halo_send, halo_recv, mode_send, mode_recv,
    share_send, share_recv, total_send, total_recv,
):
    tiles, nnz, size = a_ref.shape[0], a_ref.shape[1], a_ref.shape[2]
    modes = x_hbm.shape[0]
    width = 2 * modes
    slots = rows.shape[1]
    steps = parts.bit_length() - 1
    tables = [(cols_hbm, cols), (rows_hbm, rows), (low_hbm, low_ref), (high_hbm, high_ref)]
    tables = [pltpu.make_async_copy(*pair, x_sem.at[1 + i]) for i, pair in enumerate(tables)]
    chunks = mode_send.shape[0]
    p = lax.axis_index("dof")
    my = lax.axis_index("mode")
    has_low = p > 0
    has_up = p < parts - 1

    odd = lax.rem(p, 2)
    mate = p + 1 - 2 * odd
    far = p - 1 + 2 * odd
    has_far = (far >= 0) & (far < parts)
    far_slot = lax.rem(far + parts, parts)

    fetch = pltpu.make_async_copy(x_hbm, x_ref, x_sem.at[0])
    fetch.start()
    for table in tables:
        table.start()
    loads = []
    a_parts = a_sem.shape[0]
    span = tiles // a_parts
    for i in range(a_parts):
        view = pl.ds(i * span, span)
        loads.append(pltpu.make_async_copy(a_hbm.at[view], a_ref.at[view], a_sem.at[i]))
    for load in loads[:2]:
        load.start()

    def peer(shift, other_mode):
        place = p + shift
        place = jnp.where(place >= parts, place - parts, place)
        return place, 1 - my if other_mode else my

    near_first = sorted(
        ((d, e) for d in range(parts) for e in range(2) if d or e),
        key=lambda pair: (min(pair[0], parts - pair[0]), pair[1]),
    )
    def flipped(bit):
        return p + bit * (1 - 2 * ((p // bit) % 2))

    partners = [(flipped(1 << b), my) for b in range(steps)] + [(p, 1 - my)]
    barrier = pltpu.get_barrier_semaphore()

    @pl.when(has_far)
    def _():
        pl.semaphore_signal(barrier, inc=1, device_id=(far_slot, my), device_id_type=MESH)

    for partner in partners:
        pl.semaphore_signal(barrier, inc=1, device_id=partner, device_id_type=MESH)

    def spread(stage):
        if stage > 0:
            pl.semaphore_wait(spread_sem.at[stage - 1], 1)
        if stage < len(partners):
            pl.semaphore_signal(
                spread_sem.at[stage], inc=1, device_id=partners[stage], device_id_type=MESH
            )

    fetch.wait()
    for load in loads[2:]:
        load.start()
    for table in tables:
        table.wait()

    for t in range(tiles):
        plain[t] = x_ref[:, t * size : (t + 1) * size]
    for s in range(slots):
        for which, row in enumerate((rows[odd, s], rows[1 - odd, s])):
            sends[0, which, s] = plain[row]

    @pl.when(p == 0)
    def _():
        for level in (level0, level1, level2):
            level[tiles : tiles + slots] = jnp.zeros((slots, modes, size), jnp.bfloat16)

    @pl.when(p == parts - 1)
    def _():
        for level in (level0, level1, level2):
            level[tiles + slots :] = jnp.zeros((slots, modes, size), jnp.bfloat16)

    pl.semaphore_wait(barrier, len(partners) + has_far.astype(jnp.int32))
    spread(0)

    def halo(index, level, which):
        hop = 1 - odd if which == 2 else odd
        count = slots if which == 2 else slots // 2
        first_slot = slots // 2 if which == 1 else 0
        return pltpu.make_async_remote_copy(
            src_ref=sends.at[index, which // 2, pl.ds(first_slot, count)],
            dst_ref=level.at[pl.ds(tiles + slots * (1 - hop) + first_slot, count)],
            send_sem=halo_send.at[index, which],
            recv_sem=halo_recv.at[index, which],
            device_id=(mate if which == 2 else far_slot, my),
            device_id_type=MESH,
        )

    def start_far(index, level, which):
        pl.when(has_far)(halo(index, level, which).start)

    def start_near(index, level):
        halo(index, level, 2).start()

    def wait_halo(index, level):
        near = halo(index, level, 2)
        near.wait_recv()
        near.wait_send()
        for which in range(2):
            copy = halo(index, level, which)
            pl.when(has_far)(copy.wait_recv)
            pl.when(has_far)(copy.wait_send)

    start_far(0, level0, 0)
    start_far(0, level0, 1)
    start_near(0, level0)
    for t in range(tiles):
        level0[t] = plain[t]

    center = (high_ref[0] + low_ref[0]) * 0.5
    half_width = (high_ref[0] - low_ref[0]) * 0.5
    scale = jnp.ones((1, size), jnp.float32) / jnp.full((1, size), half_width, jnp.float32)

    def product(level, t):
        field = jnp.concatenate([level[cols[k, t]] for k in range(nnz)], axis=1)
        return lax.dot_general(field, turned[t], NN, preferred_element_type=jnp.float32)

    def first(t):
        own = level0[t].astype(jnp.float32)
        return ((product(level0, t) - center * own) * scale).astype(jnp.bfloat16)

    def second(t):
        own = level1[t].astype(jnp.float32)
        before = level0[t].astype(jnp.float32)
        return (2.0 * (product(level1, t) - center * own) * scale - before).astype(jnp.bfloat16)

    def send_tiles(index, level, make):
        for which in range(2):
            begin = which * (slots // 2)
            made = [make(rows[odd, begin + u]) for u in range(slots // 2)]
            for u, value in enumerate(made):
                sends[index, 0, begin + u] = value
            start_far(index, level, which)
        made = [make(rows[1 - odd, u]) for u in range(slots)]
        for u, value in enumerate(made):
            sends[index, 1, u] = value
        start_near(index, level)

    def all_tiles(make, target, begin, count, group=GROUP):
        group = min(group, count)

        @pl.loop(0, count // group)
        def _(i):
            made = [make(begin + i * group + u) for u in range(group)]
            for u in range(group):
                target[begin + i * group + u] = made[u]

    for i, load in enumerate(loads):
        load.wait()

        @pl.loop(0, span // 2)
        def _(j):
            for u in range(2):
                t = i * span + j * 2 + u
                for k in range(nnz):
                    turned[t, k * size : (k + 1) * size] = a_ref[t, k].T

    spread(1)
    wait_halo(0, level0)
    send_tiles(1, level1, first)
    spread(2)
    all_tiles(first, level1, 0, tiles)
    spread(3)
    wait_halo(1, level1)
    half = tiles // 2
    quarter = half // 4
    pieces = [(0, quarter), (quarter, quarter), (2 * quarter, 2 * quarter)]
    pieces = [(0, *piece) for piece in pieces] + [(1, 0, half // 2), (1, half // 2, half // 2)]
    urgent = range(3)
    later = range(3, 5)

    def exchange(c, sender):
        which, offset, count = pieces[c]
        begin = (sender if which == 0 else 1 - sender) * half + offset
        span = pl.ds(begin, count)
        return pltpu.make_async_remote_copy(
            src_ref=level2.at[span],
            dst_ref=other.at[span],
            send_sem=mode_send.at[c],
            recv_sem=mode_recv.at[c],
            device_id=(p, 1 - my),
            device_id_type=MESH,
        )

    def exchanged(c):
        which, offset, count = pieces[c]
        begin = (my if which == 0 else 1 - my) * half + offset
        all_tiles(second, level2, begin, count)
        exchange(c, my).start()

    block = shares.shape[2]
    base = (parts - 8) // 2

    def owners(k):
        return [base + b for b in range(8)] if k == 2 else [base + k % 2 + 2 * b for b in range(4)]

    def owned(k):
        place = p - base
        inside = (place >= 0) & (place < 8)
        return inside if k == 2 else inside & (lax.rem(p - base + parts, 2) == k % 2)

    def blocks_wait(ref, count, sem):
        view = ref.at[pl.ds(0, count)]
        pltpu.make_async_copy(view, view, sem).wait()

    def share(k, value):
        for b, owner in enumerate(owners(k)):
            shares[k, b] = value[b * block : (b + 1) * block]
        for b, owner in enumerate(owners(k)):
            copy = pltpu.make_async_remote_copy(
                src_ref=shares.at[k, b],
                dst_ref=gathered.at[k * parts + p],
                send_sem=share_send.at[k],
                recv_sem=share_recv.at[k],
                device_id=(owner, my),
                device_id_type=MESH,
            )
            pl.when(p != owner)(copy.start)

            @pl.when(p == owner)
            def _():
                gathered[k * parts + p] = shares[k, b]

    def total(k):
        count = len(owners(k))

        @pl.when(owned(k))
        def _():
            blocks_wait(gathered, parts - 1, share_recv.at[k])
            value = gathered[k * parts]
            for q in range(1, parts):
                value = value + gathered[k * parts + q]
            sums[k] = value
            slot = my * count + (p - base) // (8 // count)
            totals[k, slot] = value

            for shift, other_mode in reversed(near_first):
                pltpu.make_async_remote_copy(
                    src_ref=sums.at[k],
                    dst_ref=totals.at[k, slot],
                    send_sem=total_send.at[k],
                    recv_sem=total_recv.at[k],
                    device_id=peer(shift, other_mode),
                    device_id_type=MESH,
                ).start()

    def arrived(k):
        count = len(owners(k))

        @pl.when(owned(k))
        def _():
            blocks_wait(totals.at[k], 2 * count - 1, total_recv.at[k])

        @pl.when(jnp.logical_not(owned(k)))
        def _():
            blocks_wait(totals.at[k], 2 * count, total_recv.at[k])

        flat = totals[k, : 2 * count].reshape(2, count * block, width) / (parts * tiles * size)
        return flat[0], flat[1]

    def sent(k):
        count = len(owners(k))

        @pl.when(owned(k))
        def _():
            blocks_wait(shares.at[k], count - 1, share_send.at[k])
            blocks_wait(gathered, 2 * parts - 1, total_send.at[k])

        @pl.when(jnp.logical_not(owned(k)))
        def _():
            blocks_wait(shares.at[k], count, share_send.at[k])

    def contract(left, right, begin, count):
        acc = jnp.zeros((modes, modes), jnp.float32)
        for i in range(0, count, 8):
            lhs = jnp.concatenate([left[begin + i + u] for u in range(8)], axis=1)
            rhs = jnp.concatenate([right[begin + i + u] for u in range(8)], axis=1)
            acc = acc + lax.dot_general(lhs, rhs, NT, preferred_element_type=jnp.float32)
        return acc

    def fold(value):
        return jnp.concatenate([value[: modes // 2], value[modes // 2 :]], axis=1)

    def unfold(value):
        return jnp.concatenate([value[:, :modes], value[:, modes:]], axis=0)

    for c in urgent:
        exchanged(c)
    spread(4)
    send_tiles(2, level2, second)
    for c in later:
        exchanged(c)
    for stage in range(5, len(partners) + 1):
        spread(stage)
    share(0, fold(contract(level2, level2, 0, tiles)))
    wait_halo(2, level2)
    all_tiles(lambda t: product(level2, t).astype(jnp.bfloat16), image, 0, tiles)
    for c in urgent:
        exchange(c, 1 - my).wait_recv()
    cross = contract(level2, other, (1 - my) * half, half)
    share(1, fold(jnp.where(my == 0, cross, cross.T)))
    total(0)
    own_projected = contract(image, level2, 0, tiles)
    mixed = contract(image, other, (1 - my) * half, half)
    pair = jnp.concatenate([own_projected, mixed], axis=1)
    share(2, jnp.where(my == 0, pair, pltpu.roll(pair, modes, 1)))
    total(1)
    rest_begin = my * half
    exchange(3, 1 - my).wait_recv()
    mixed = contract(image, other, rest_begin, half // 2)
    exchange(4, 1 - my).wait_recv()
    share(3, fold(mixed + contract(image, other, rest_begin + half // 2, half // 2)))

    step = 16
    row_id = lax.broadcasted_iota(jnp.int32, (modes, modes), 0)
    col_id = lax.broadcasted_iota(jnp.int32, (modes, modes), 1)
    small = lax.broadcasted_iota(jnp.int32, (step, 1), 0)
    lanes = lax.broadcasted_iota(jnp.int32, (step, width), 1)

    def exact(left, right, dims):
        return lax.dot_general(
            left, right, dims, precision=EXACT, preferred_element_type=jnp.float32
        )

    def factor_inverse(gram):
        eye = (row_id == col_id).astype(jnp.float32)
        work[...] = jnp.concatenate([gram, eye], axis=1)

        @pl.loop(0, modes // step)
        def _(b):
            begin = pl.multiple_of(b * step, step)
            panel = work[pl.ds(begin, step), :]
            near = panel
            columns = [
                jnp.sum(jnp.where(lanes == begin + s, near, 0.0), axis=1, keepdims=True)
                for s in range(step)
            ]
            pivots = jnp.zeros((step, 1), jnp.float32)
            for q in range(step):
                pivot = columns[q][q : q + 1, :]
                pivots = jnp.where(small == q, pivot, pivots)
                if q == step - 1:
                    break
                factor = jnp.where(small > q, columns[q] / pivot, 0.0)
                panel = panel - factor * panel[q : q + 1, :]
                for s in range(q + 1, step):
                    columns[s] = columns[s] - factor * columns[s][q : q + 1, :]
            inv_ref[pl.ds(begin, step), :] = panel / jnp.sqrt(pivots)
            ahead = (lanes >= begin + step) & (lanes < modes)
            below = jnp.where(ahead, panel / pivots, 0.0)[:, :modes]
            work[...] = work[...] - exact(below, panel, TN)

        return inv_ref[...][:, modes:]

    total(2)
    gram0, gram1 = arrived(0)
    gram0, gram1 = unfold(gram0), unfold(gram1)
    inv00 = factor_inverse(gram0)
    cross0, cross1 = arrived(1)
    bridge = exact(inv00, unfold(cross0 + cross1), NN)
    rest = gram1 - exact(bridge, bridge, TN)
    turn = exact(bridge, inv00, TN)
    total(3)
    inv11 = factor_inverse(rest)
    inv10 = -exact(inv11, turn, NN)
    lower = jnp.concatenate([inv10, inv11], axis=1)
    blank = jnp.zeros((modes, modes), jnp.float32)
    upper = jnp.concatenate([inv00, blank], axis=1)
    inverse = jnp.concatenate([upper, lower], axis=0)
    own = jnp.where(my == 0, upper, pltpu.roll(lower, modes, 1))
    inv_t[...] = own.astype(jnp.bfloat16)
    for t in range(0, tiles, 2):
        two = jnp.concatenate(
            [jnp.concatenate([level2[u], other[u]], axis=0) for u in (t, t + 1)], axis=1
        )
        basis[:, t * size : (t + 2) * size] = lax.dot_general(
            inv_t[...], two, NN, preferred_element_type=jnp.float32
        ).astype(jnp.bfloat16)
    keep = pltpu.make_async_copy(basis, basis_ref, keep_sem.at[0])
    keep.start()
    projected_t = jnp.concatenate(arrived(2), axis=0)
    late0, late1 = arrived(3)
    projected_t = projected_t + jnp.concatenate(
        [
            jnp.concatenate([blank, unfold(late0)], axis=1),
            jnp.concatenate([unfold(late1), blank], axis=1),
        ],
        axis=0,
    )
    ritz_ref[...] = exact(exact(inverse, projected_t, NT), inverse, NT)
    keep.wait()
    for c in range(chunks):
        exchange(c, my).wait_send()
    for k in range(4):
        sent(k)


def finish(basis_in, ritz_in, basis_ref, ritz_ref, sem):
    copies = [
        pltpu.make_async_copy(basis_in, basis_ref, sem.at[0]),
        pltpu.make_async_copy(ritz_in, ritz_ref, sem.at[1]),
    ]
    for copy in copies:
        copy.start()
    for copy in copies:
        copy.wait()


def shards(parts, stiffness_tiles, tile_cols, send_rows, block, lower_bound, upper_bound):
    row_count, modes = block.shape
    tiles, nnz, size = stiffness_tiles.shape[:3]
    slots = send_rows.shape[1]
    width = 2 * modes
    assert parts >= 16 and parts & (parts - 1) == 0
    chunks = 5
    vmem = pl.BlockSpec(memory_space=pltpu.VMEM)
    hbm = pl.BlockSpec(memory_space=pl.ANY)
    far = pl.BlockSpec(memory_space=pltpu.HBM)
    dma = pltpu.SemaphoreType.DMA
    level = pltpu.VMEM((tiles + 2 * slots, modes, size), jnp.bfloat16)
    field = pltpu.VMEM((tiles, modes, size), jnp.bfloat16)
    basis, ritz = pl.pallas_call(
        functools.partial(kernel, parts),
        out_shape=(
            jax.ShapeDtypeStruct((modes, row_count), jnp.bfloat16),
            jax.ShapeDtypeStruct((width, width), jnp.float32),
        ),
        in_specs=[far] * 6,
        out_specs=(hbm, vmem),
        scratch_shapes=[
            pltpu.VMEM(stiffness_tiles.shape, jnp.bfloat16),
            pltpu.VMEM((tiles, nnz * size, size), jnp.bfloat16),
            level, level, level, pltpu.VMEM((modes, row_count), jnp.bfloat16), field, field, field,
            pltpu.VMEM((3, 2, slots, modes, size), jnp.bfloat16),
            pltpu.VMEM((4, 8, 8, width), jnp.float32),
            pltpu.VMEM((4 * parts, 8, width), jnp.float32),
            pltpu.VMEM((4, 16, 8, width), jnp.float32),
            pltpu.VMEM((4, 8, width), jnp.float32),
            pltpu.VMEM((modes, width), jnp.float32),
            pltpu.VMEM((modes, width), jnp.float32),
            pltpu.VMEM((modes, width), jnp.bfloat16),
            pltpu.VMEM((modes, row_count), jnp.bfloat16),
            pltpu.SMEM((nnz, tiles), jnp.int32),
            pltpu.SMEM(send_rows.shape, jnp.int32),
            pltpu.SMEM((1,), jnp.float32),
            pltpu.SMEM((1,), jnp.float32),
            pltpu.SemaphoreType.REGULAR((parts.bit_length(),)),
            dma((5,)), dma((8,)), dma((1,)), dma((3, 3)), dma((3, 3)), dma((chunks,)), dma((chunks,)),
            dma((4,)), dma((4,)), dma((4,)), dma((4,)),
        ],
        compiler_params=pltpu.CompilerParams(
            collective_id=0, has_side_effects=True, vmem_limit_bytes=50331648
        ),
    )(
        *[pltpu.with_memory_space_constraint(ref, pltpu.HBM) for ref in (tile_cols.T, send_rows)],
        lower_bound, upper_bound,
        *[pltpu.with_memory_space_constraint(ref, pltpu.HBM) for ref in (block.T, stiffness_tiles)],
    )
    basis, ritz = pl.pallas_call(
        finish,
        out_shape=(
            jax.ShapeDtypeStruct((modes, row_count), jnp.bfloat16),
            jax.ShapeDtypeStruct((width, width), jnp.float32),
        ),
        in_specs=[hbm, hbm],
        out_specs=(hbm, hbm),
        scratch_shapes=[dma((2,))],
        compiler_params=pltpu.CompilerParams(vmem_limit_bytes=8 * 1024 * 1024),
    )(basis, ritz)
    return basis.T, ritz


def solution(mesh):
    placed = (
        P("dof", None, None, None),
        P("dof", None),
        P("dof", None),
        P("dof", "mode"),
        P(),
        P(),
    )
    return jax.shard_map(
        functools.partial(shards, mesh.shape["dof"]),
        mesh=mesh, in_specs=placed, out_specs=(P("dof", "mode"), P()), check_vma=False,
    )
```

```python
import functools

import jax
import jax.numpy as jnp
from jax import lax
from jax.experimental import pallas as pl
from jax.experimental.pallas import tpu as pltpu
from jax.sharding import PartitionSpec as P

MESH = pl.DeviceIdType.MESH
GROUP = 16
NT = (((1,), (1,)), ((), ()))
NN = (((1,), (0,)), ((), ()))
TN = (((0,), (0,)), ((), ()))
EXACT = lax.Precision.HIGHEST


def kernel(
    parts, cols_hbm, rows_hbm, low_hbm, high_hbm, x_hbm, a_hbm, basis_ref, ritz_ref,
    a_ref, turned, level0, level1, level2, x_ref, plain, image, other, sends,
    shares, gathered, totals, sums, work, inv_ref, inv_t, basis,
    cols, rows, low_ref, high_ref, spread_sem, x_sem, a_sem, keep_sem, halo_send, halo_recv, mode_send, mode_recv,
    share_send, share_recv, total_send, total_recv,
):
    tiles, nnz, size = a_ref.shape[0], a_ref.shape[1], a_ref.shape[2]
    modes = x_hbm.shape[0]
    width = 2 * modes
    slots = rows.shape[1]
    steps = parts.bit_length() - 1
    pieces_far = halo_send.shape[1] - 1
    tables = [(cols_hbm, cols), (rows_hbm, rows), (low_hbm, low_ref), (high_hbm, high_ref)]
    tables = [pltpu.make_async_copy(*pair, x_sem.at[1 + i]) for i, pair in enumerate(tables)]
    chunks = mode_send.shape[0]
    p = lax.axis_index("dof")
    my = lax.axis_index("mode")
    has_low = p > 0
    has_up = p < parts - 1

    odd = lax.rem(p, 2)
    mate = p + 1 - 2 * odd
    far = p - 1 + 2 * odd
    has_far = (far >= 0) & (far < parts)
    far_slot = lax.rem(far + parts, parts)

    fetch = pltpu.make_async_copy(x_hbm, x_ref, x_sem.at[0])
    fetch.start()
    for table in tables:
        table.start()
    loads = []
    a_parts = a_sem.shape[0]
    span = tiles // a_parts
    for i in range(a_parts):
        view = pl.ds(i * span, span)
        loads.append(pltpu.make_async_copy(a_hbm.at[view], a_ref.at[view], a_sem.at[i]))
    for load in loads[:2]:
        load.start()

    def peer(shift, other_mode):
        place = p + shift
        place = jnp.where(place >= parts, place - parts, place)
        return place, 1 - my if other_mode else my

    near_first = sorted(
        ((d, e) for d in range(parts) for e in range(2) if d or e),
        key=lambda pair: (min(pair[0], parts - pair[0]), pair[1]),
    )
    def flipped(bit):
        return p + bit * (1 - 2 * ((p // bit) % 2))

    partners = [(flipped(1 << b), my) for b in range(steps)] + [(p, 1 - my)]
    barrier = pltpu.get_barrier_semaphore()

    @pl.when(has_far)
    def _():
        pl.semaphore_signal(barrier, inc=1, device_id=(far_slot, my), device_id_type=MESH)

    for partner in partners:
        pl.semaphore_signal(barrier, inc=1, device_id=partner, device_id_type=MESH)

    def spread(stage):
        if stage > 0:
            pl.semaphore_wait(spread_sem.at[stage - 1], 1)
        if stage < len(partners):
            pl.semaphore_signal(
                spread_sem.at[stage], inc=1, device_id=partners[stage], device_id_type=MESH
            )

    fetch.wait()
    for load in loads[2:]:
        load.start()
    for table in tables:
        table.wait()

    for t in range(tiles):
        plain[t] = x_ref[:, t * size : (t + 1) * size]
    for s in range(slots):
        for which, row in enumerate((rows[odd, s], rows[1 - odd, s])):
            sends[0, which, s] = plain[row]

    @pl.when(p == 0)
    def _():
        for level in (level0, level1, level2):
            level[tiles : tiles + slots] = jnp.zeros((slots, modes, size), jnp.bfloat16)

    @pl.when(p == parts - 1)
    def _():
        for level in (level0, level1, level2):
            level[tiles + slots :] = jnp.zeros((slots, modes, size), jnp.bfloat16)

    pl.semaphore_wait(barrier, len(partners) + has_far.astype(jnp.int32))
    spread(0)

    def halo(index, level, which):
        near = which == pieces_far
        hop = 1 - odd if near else odd
        count = slots if near else slots // pieces_far
        first_slot = 0 if near else which * count
        return pltpu.make_async_remote_copy(
            src_ref=sends.at[index, int(near), pl.ds(first_slot, count)],
            dst_ref=level.at[pl.ds(tiles + slots * (1 - hop) + first_slot, count)],
            send_sem=halo_send.at[index, which],
            recv_sem=halo_recv.at[index, which],
            device_id=(mate if near else far_slot, my),
            device_id_type=MESH,
        )

    def start_far(index, level, which):
        pl.when(has_far)(halo(index, level, which).start)

    def start_near(index, level):
        halo(index, level, pieces_far).start()

    def wait_halo(index, level):
        near = halo(index, level, pieces_far)
        near.wait_recv()
        near.wait_send()
        for which in range(pieces_far):
            copy = halo(index, level, which)
            pl.when(has_far)(copy.wait_recv)
            pl.when(has_far)(copy.wait_send)

    for which in range(pieces_far):
        start_far(0, level0, which)
    start_near(0, level0)
    for t in range(tiles):
        level0[t] = plain[t]

    center = (high_ref[0] + low_ref[0]) * 0.5
    half_width = (high_ref[0] - low_ref[0]) * 0.5
    scale = jnp.ones((1, size), jnp.float32) / jnp.full((1, size), half_width, jnp.float32)

    def product(level, t):
        field = jnp.concatenate([level[cols[k, t]] for k in range(nnz)], axis=1)
        return lax.dot_general(field, turned[t], NN, preferred_element_type=jnp.float32)

    def first(t):
        own = level0[t].astype(jnp.float32)
        return ((product(level0, t) - center * own) * scale).astype(jnp.bfloat16)

    def second(t):
        own = level1[t].astype(jnp.float32)
        before = level0[t].astype(jnp.float32)
        return (2.0 * (product(level1, t) - center * own) * scale - before).astype(jnp.bfloat16)

    def send_tiles(index, level, make):
        count = slots // pieces_far
        for which in range(pieces_far):
            made = [make(rows[odd, which * count + u]) for u in range(count)]
            for u, value in enumerate(made):
                sends[index, 0, which * count + u] = value
            start_far(index, level, which)
        made = [make(rows[1 - odd, u]) for u in range(slots)]
        for u, value in enumerate(made):
            sends[index, 1, u] = value
        start_near(index, level)

    def all_tiles(make, target, begin, count, group=GROUP):
        group = min(group, count)

        @pl.loop(0, count // group)
        def _(i):
            made = [make(begin + i * group + u) for u in range(group)]
            for u in range(group):
                target[begin + i * group + u] = made[u]

    for i, load in enumerate(loads):
        load.wait()

        @pl.loop(0, span // 2)
        def _(j):
            for u in range(2):
                t = i * span + j * 2 + u
                for k in range(nnz):
                    turned[t, k * size : (k + 1) * size] = a_ref[t, k].T

    spread(1)
    wait_halo(0, level0)
    send_tiles(1, level1, first)
    spread(2)
    all_tiles(first, level1, 0, tiles)
    spread(3)
    wait_halo(1, level1)
    half = tiles // 2
    quarter = half // 4
    pieces = [(0, quarter), (quarter, quarter), (2 * quarter, 2 * quarter)]
    pieces = [(0, *piece) for piece in pieces] + [(1, 0, half // 2), (1, half // 2, half // 2)]
    urgent = range(3)
    later = range(3, 5)

    def exchange(c, sender):
        which, offset, count = pieces[c]
        begin = (sender if which == 0 else 1 - sender) * half + offset
        span = pl.ds(begin, count)
        return pltpu.make_async_remote_copy(
            src_ref=level2.at[span],
            dst_ref=other.at[span],
            send_sem=mode_send.at[c],
            recv_sem=mode_recv.at[c],
            device_id=(p, 1 - my),
            device_id_type=MESH,
        )

    def exchanged(c):
        which, offset, count = pieces[c]
        begin = (my if which == 0 else 1 - my) * half + offset
        all_tiles(second, level2, begin, count)
        exchange(c, my).start()

    block = shares.shape[2]
    base = (parts - 8) // 2

    def owners(k):
        return [base + k % 2 + 2 * b for b in range(4)]

    def owned(k):
        place = p - base
        inside = (place >= 0) & (place < 8)
        return inside & (lax.rem(place + parts, 2) == k % 2)

    def blocks_wait(ref, count, sem):
        view = ref.at[pl.ds(0, count)]
        pltpu.make_async_copy(view, view, sem).wait()

    def share(k, value):
        for b, owner in enumerate(owners(k)):
            shares[k, b] = value[b * block : (b + 1) * block]
        for b, owner in enumerate(owners(k)):
            copy = pltpu.make_async_remote_copy(
                src_ref=shares.at[k, b],
                dst_ref=gathered.at[k * parts + p],
                send_sem=share_send.at[k],
                recv_sem=share_recv.at[k],
                device_id=(owner, my),
                device_id_type=MESH,
            )
            pl.when(p != owner)(copy.start)

            @pl.when(p == owner)
            def _():
                gathered[k * parts + p] = shares[k, b]

    def total(k):
        count = len(owners(k))

        @pl.when(owned(k))
        def _():
            blocks_wait(gathered, parts - 1, share_recv.at[k])
            value = gathered[k * parts]
            for q in range(1, parts):
                value = value + gathered[k * parts + q]
            sums[k] = value
            slot = my * count + (p - base) // (8 // count)
            totals[k, slot] = value

            for shift, other_mode in reversed(near_first):
                pltpu.make_async_remote_copy(
                    src_ref=sums.at[k],
                    dst_ref=totals.at[k, slot],
                    send_sem=total_send.at[k],
                    recv_sem=total_recv.at[k],
                    device_id=peer(shift, other_mode),
                    device_id_type=MESH,
                ).start()

    def arrived(k):
        count = len(owners(k))

        @pl.when(owned(k))
        def _():
            blocks_wait(totals.at[k], 2 * count - 1, total_recv.at[k])

        @pl.when(jnp.logical_not(owned(k)))
        def _():
            blocks_wait(totals.at[k], 2 * count, total_recv.at[k])

        flat = totals[k, : 2 * count].reshape(2, count * block, width) / (parts * tiles * size)
        return flat[0], flat[1]

    def sent(k):
        count = len(owners(k))

        @pl.when(owned(k))
        def _():
            blocks_wait(shares.at[k], count - 1, share_send.at[k])
            blocks_wait(gathered, 2 * parts - 1, total_send.at[k])

        @pl.when(jnp.logical_not(owned(k)))
        def _():
            blocks_wait(shares.at[k], count, share_send.at[k])

    def contract(left, right, begin, count):
        acc = jnp.zeros((modes, modes), jnp.float32)
        for i in range(0, count, 8):
            lhs = jnp.concatenate([left[begin + i + u] for u in range(8)], axis=1)
            rhs = jnp.concatenate([right[begin + i + u] for u in range(8)], axis=1)
            acc = acc + lax.dot_general(lhs, rhs, NT, preferred_element_type=jnp.float32)
        return acc

    def fold(value):
        return jnp.concatenate([value[: modes // 2], value[modes // 2 :]], axis=1)

    def unfold(value):
        return jnp.concatenate([value[:, :modes], value[:, modes:]], axis=0)

    for c in urgent:
        exchanged(c)
    spread(4)
    send_tiles(2, level2, second)
    for c in later:
        exchanged(c)
    for stage in range(5, len(partners) + 1):
        spread(stage)
    share(0, fold(contract(level2, level2, 0, tiles)))
    wait_halo(2, level2)
    all_tiles(lambda t: product(level2, t).astype(jnp.bfloat16), image, 0, tiles)
    share(2, fold(contract(image, level2, 0, tiles)))
    for c in urgent:
        exchange(c, 1 - my).wait_recv()
    cross = contract(level2, other, (1 - my) * half, half)
    share(1, fold(jnp.where(my == 0, cross, cross.T)))
    mixed = contract(image, other, (1 - my) * half, half)
    total(0)
    total(1)
    rest_begin = my * half
    exchange(3, 1 - my).wait_recv()
    mixed = mixed + contract(image, other, rest_begin, half // 2)
    exchange(4, 1 - my).wait_recv()
    share(3, fold(mixed + contract(image, other, rest_begin + half // 2, half // 2)))

    step = 16
    row_id = lax.broadcasted_iota(jnp.int32, (modes, modes), 0)
    col_id = lax.broadcasted_iota(jnp.int32, (modes, modes), 1)
    small = lax.broadcasted_iota(jnp.int32, (step, 1), 0)
    lanes = lax.broadcasted_iota(jnp.int32, (step, width), 1)

    def exact(left, right, dims):
        return lax.dot_general(
            left, right, dims, precision=EXACT, preferred_element_type=jnp.float32
        )

    def factor_inverse(gram):
        eye = (row_id == col_id).astype(jnp.float32)
        work[...] = jnp.concatenate([gram, eye], axis=1)

        @pl.loop(0, modes // step)
        def _(b):
            begin = pl.multiple_of(b * step, step)
            panel = work[pl.ds(begin, step), :]
            near = panel
            columns = [
                jnp.sum(jnp.where(lanes == begin + s, near, 0.0), axis=1, keepdims=True)
                for s in range(step)
            ]
            pivots = jnp.zeros((step, 1), jnp.float32)
            for q in range(step):
                pivot = columns[q][q : q + 1, :]
                pivots = jnp.where(small == q, pivot, pivots)
                if q == step - 1:
                    break
                factor = jnp.where(small > q, columns[q] / pivot, 0.0)
                panel = panel - factor * panel[q : q + 1, :]
                for s in range(q + 1, step):
                    columns[s] = columns[s] - factor * columns[s][q : q + 1, :]
            inv_ref[pl.ds(begin, step), :] = panel / jnp.sqrt(pivots)
            ahead = (lanes >= begin + step) & (lanes < modes)
            below = jnp.where(ahead, panel / pivots, 0.0)[:, :modes]
            work[...] = work[...] - exact(below, panel, TN)

        return inv_ref[...][:, modes:]

    total(2)
    gram0, gram1 = arrived(0)
    gram0, gram1 = unfold(gram0), unfold(gram1)
    inv00 = factor_inverse(gram0)
    cross0, cross1 = arrived(1)
    bridge = exact(inv00, unfold(cross0 + cross1), NN)
    rest = gram1 - exact(bridge, bridge, TN)
    turn = exact(bridge, inv00, TN)
    total(3)
    inv11 = factor_inverse(rest)
    inv10 = -exact(inv11, turn, NN)
    lower = jnp.concatenate([inv10, inv11], axis=1)
    blank = jnp.zeros((modes, modes), jnp.float32)
    upper = jnp.concatenate([inv00, blank], axis=1)
    inverse = jnp.concatenate([upper, lower], axis=0)
    own = jnp.where(my == 0, upper, pltpu.roll(lower, modes, 1))
    inv_t[...] = own.astype(jnp.bfloat16)
    for t in range(0, tiles, 2):
        two = jnp.concatenate(
            [jnp.concatenate([level2[u], other[u]], axis=0) for u in (t, t + 1)], axis=1
        )
        basis[:, t * size : (t + 2) * size] = lax.dot_general(
            inv_t[...], two, NN, preferred_element_type=jnp.float32
        ).astype(jnp.bfloat16)
    keep = pltpu.make_async_copy(basis, basis_ref, keep_sem.at[0])
    keep.start()
    own0, own1 = arrived(2)
    late0, late1 = arrived(3)
    projected_t = jnp.concatenate(
        [
            jnp.concatenate([unfold(own0), unfold(late0)], axis=1),
            jnp.concatenate([unfold(late1), unfold(own1)], axis=1),
        ],
        axis=0,
    )
    ritz_ref[...] = exact(exact(inverse, projected_t, NT), inverse, NT)
    keep.wait()
    for c in range(chunks):
        exchange(c, my).wait_send()
    for k in range(4):
        sent(k)


def finish(basis_in, ritz_in, basis_ref, ritz_ref, sem):
    copies = [
        pltpu.make_async_copy(basis_in, basis_ref, sem.at[0]),
        pltpu.make_async_copy(ritz_in, ritz_ref, sem.at[1]),
    ]
    for copy in copies:
        copy.start()
    for copy in copies:
        copy.wait()


def shards(parts, stiffness_tiles, tile_cols, send_rows, block, lower_bound, upper_bound):
    row_count, modes = block.shape
    tiles, nnz, size = stiffness_tiles.shape[:3]
    slots = send_rows.shape[1]
    width = 2 * modes
    assert parts >= 16 and parts & (parts - 1) == 0
    chunks = 5
    vmem = pl.BlockSpec(memory_space=pltpu.VMEM)
    hbm = pl.BlockSpec(memory_space=pl.ANY)
    far = pl.BlockSpec(memory_space=pltpu.HBM)
    dma = pltpu.SemaphoreType.DMA
    level = pltpu.VMEM((tiles + 2 * slots, modes, size), jnp.bfloat16)
    field = pltpu.VMEM((tiles, modes, size), jnp.bfloat16)
    basis, ritz = pl.pallas_call(
        functools.partial(kernel, parts),
        out_shape=(
            jax.ShapeDtypeStruct((modes, row_count), jnp.bfloat16),
            jax.ShapeDtypeStruct((width, width), jnp.float32),
        ),
        in_specs=[far] * 6,
        out_specs=(hbm, vmem),
        scratch_shapes=[
            pltpu.VMEM(stiffness_tiles.shape, jnp.bfloat16),
            pltpu.VMEM((tiles, nnz * size, size), jnp.bfloat16),
            level, level, level, pltpu.VMEM((modes, row_count), jnp.bfloat16), field, field, field,
            pltpu.VMEM((3, 2, slots, modes, size), jnp.bfloat16),
            pltpu.VMEM((4, 4, 8, width), jnp.float32),
            pltpu.VMEM((4 * parts, 8, width), jnp.float32),
            pltpu.VMEM((4, 8, 8, width), jnp.float32),
            pltpu.VMEM((4, 8, width), jnp.float32),
            pltpu.VMEM((modes, width), jnp.float32),
            pltpu.VMEM((modes, width), jnp.float32),
            pltpu.VMEM((modes, width), jnp.bfloat16),
            pltpu.VMEM((modes, row_count), jnp.bfloat16),
            pltpu.SMEM((nnz, tiles), jnp.int32),
            pltpu.SMEM(send_rows.shape, jnp.int32),
            pltpu.SMEM((1,), jnp.float32),
            pltpu.SMEM((1,), jnp.float32),
            pltpu.SemaphoreType.REGULAR((parts.bit_length(),)),
            dma((5,)), dma((8,)), dma((1,)), dma((3, 3)), dma((3, 3)), dma((chunks,)), dma((chunks,)),
            dma((4,)), dma((4,)), dma((4,)), dma((4,)),
        ],
        compiler_params=pltpu.CompilerParams(
            collective_id=0, has_side_effects=True, vmem_limit_bytes=50331648
        ),
    )(
        *[pltpu.with_memory_space_constraint(ref, pltpu.HBM) for ref in (tile_cols.T, send_rows)],
        lower_bound, upper_bound,
        *[pltpu.with_memory_space_constraint(ref, pltpu.HBM) for ref in (block.T, stiffness_tiles)],
    )
    basis, ritz = pl.pallas_call(
        finish,
        out_shape=(
            jax.ShapeDtypeStruct((modes, row_count), jnp.bfloat16),
            jax.ShapeDtypeStruct((width, width), jnp.float32),
        ),
        in_specs=[hbm, hbm],
        out_specs=(hbm, hbm),
        scratch_shapes=[dma((2,))],
        compiler_params=pltpu.CompilerParams(vmem_limit_bytes=8 * 1024 * 1024),
    )(basis, ritz)
    return basis.T, ritz


def solution(mesh):
    placed = (
        P("dof", None, None, None),
        P("dof", None),
        P("dof", None),
        P("dof", "mode"),
        P(),
        P(),
    )
    return jax.shard_map(
        functools.partial(shards, mesh.shape["dof"]),
        mesh=mesh, in_specs=placed, out_specs=(P("dof", "mode"), P()), check_vma=False,
    )
```

```python
import functools

import jax
import jax.numpy as jnp
from jax import lax
from jax.experimental import pallas as pl
from jax.experimental.pallas import tpu as pltpu
from jax.sharding import PartitionSpec as P

MESH = pl.DeviceIdType.MESH
GROUP = 16
NT = (((1,), (1,)), ((), ()))
NN = (((1,), (0,)), ((), ()))
TN = (((0,), (0,)), ((), ()))
EXACT = lax.Precision.HIGHEST


def kernel(
    parts, cols_hbm, rows_hbm, low_hbm, high_hbm, x_hbm, a_hbm, basis_ref, ritz_ref,
    a_ref, turned, level0, level1, level2, x_ref, plain, image, other, sends,
    shares, gathered, totals, sums, work, inv_ref, inv_t, basis,
    cols, rows, low_ref, high_ref, spread_sem, x_sem, a_sem, keep_sem, halo_send, halo_recv, mode_send, mode_recv,
    share_send, share_recv, total_send, total_recv,
):
    tiles, nnz, size = a_ref.shape[0], a_ref.shape[1], a_ref.shape[2]
    modes = x_hbm.shape[0]
    width = 2 * modes
    slots = rows.shape[1]
    steps = parts.bit_length() - 1
    pieces_far = halo_send.shape[1] - 1
    tables = [(cols_hbm, cols), (rows_hbm, rows), (low_hbm, low_ref), (high_hbm, high_ref)]
    tables = [pltpu.make_async_copy(*pair, x_sem.at[1 + i]) for i, pair in enumerate(tables)]
    chunks = mode_send.shape[0]
    p = lax.axis_index("dof")
    my = lax.axis_index("mode")
    has_low = p > 0
    has_up = p < parts - 1

    odd = lax.rem(p, 2)
    mate = p + 1 - 2 * odd
    far = p - 1 + 2 * odd
    has_far = (far >= 0) & (far < parts)
    far_slot = lax.rem(far + parts, parts)

    fetch = pltpu.make_async_copy(x_hbm, x_ref, x_sem.at[0])
    fetch.start()
    for table in tables:
        table.start()
    loads = []
    a_parts = a_sem.shape[0]
    span = tiles // a_parts
    for i in range(a_parts):
        view = pl.ds(i * span, span)
        loads.append(pltpu.make_async_copy(a_hbm.at[view], a_ref.at[view], a_sem.at[i]))
    for load in loads[:2]:
        load.start()

    def peer(shift, other_mode):
        place = p + shift
        place = jnp.where(place >= parts, place - parts, place)
        return place, 1 - my if other_mode else my

    near_first = sorted(
        ((d, e) for d in range(parts) for e in range(2) if d or e),
        key=lambda pair: (min(pair[0], parts - pair[0]), pair[1]),
    )
    def flipped(bit):
        return p + bit * (1 - 2 * ((p // bit) % 2))

    partners = [(flipped(1 << b), my) for b in range(steps)] + [(p, 1 - my)]
    barrier = pltpu.get_barrier_semaphore()

    @pl.when(has_far)
    def _():
        pl.semaphore_signal(barrier, inc=1, device_id=(far_slot, my), device_id_type=MESH)

    for partner in partners:
        pl.semaphore_signal(barrier, inc=1, device_id=partner, device_id_type=MESH)

    def spread(stage):
        if stage > 0:
            pl.semaphore_wait(spread_sem.at[stage - 1], 1)
        if stage < len(partners):
            pl.semaphore_signal(
                spread_sem.at[stage], inc=1, device_id=partners[stage], device_id_type=MESH
            )

    fetch.wait()
    for load in loads[2:]:
        load.start()
    for table in tables:
        table.wait()

    for t in range(tiles):
        plain[t] = x_ref[:, t * size : (t + 1) * size]
    for s in range(slots):
        for which, row in enumerate((rows[odd, s], rows[1 - odd, s])):
            sends[0, which, s] = plain[row]

    @pl.when(p == 0)
    def _():
        for level in (level0, level1, level2):
            level[tiles : tiles + slots] = jnp.zeros((slots, modes, size), jnp.bfloat16)

    @pl.when(p == parts - 1)
    def _():
        for level in (level0, level1, level2):
            level[tiles + slots :] = jnp.zeros((slots, modes, size), jnp.bfloat16)

    pl.semaphore_wait(barrier, len(partners) + has_far.astype(jnp.int32))
    spread(0)

    def halo(index, level, which):
        near = which == pieces_far
        hop = 1 - odd if near else odd
        count = slots if near else slots // pieces_far
        first_slot = 0 if near else which * count
        return pltpu.make_async_remote_copy(
            src_ref=sends.at[index, int(near), pl.ds(first_slot, count)],
            dst_ref=level.at[pl.ds(tiles + slots * (1 - hop) + first_slot, count)],
            send_sem=halo_send.at[index, which],
            recv_sem=halo_recv.at[index, which],
            device_id=(mate if near else far_slot, my),
            device_id_type=MESH,
        )

    def start_far(index, level, which):
        pl.when(has_far)(halo(index, level, which).start)

    def start_near(index, level):
        halo(index, level, pieces_far).start()

    def wait_halo(index, level):
        near = halo(index, level, pieces_far)
        near.wait_recv()
        near.wait_send()
        for which in range(pieces_far):
            copy = halo(index, level, which)
            pl.when(has_far)(copy.wait_recv)
            pl.when(has_far)(copy.wait_send)

    for which in range(pieces_far):
        start_far(0, level0, which)
    start_near(0, level0)
    for t in range(tiles):
        level0[t] = plain[t]

    center = (high_ref[0] + low_ref[0]) * 0.5
    half_width = (high_ref[0] - low_ref[0]) * 0.5
    scale = jnp.ones((1, size), jnp.float32) / jnp.full((1, size), half_width, jnp.float32)

    def product(level, t):
        field = jnp.concatenate([level[cols[k, t]] for k in range(nnz)], axis=1)
        return lax.dot_general(field, turned[t], NN, preferred_element_type=jnp.float32)

    def first(t):
        own = level0[t].astype(jnp.float32)
        return ((product(level0, t) - center * own) * scale).astype(jnp.bfloat16)

    def second(t):
        own = level1[t].astype(jnp.float32)
        before = level0[t].astype(jnp.float32)
        return (2.0 * (product(level1, t) - center * own) * scale - before).astype(jnp.bfloat16)

    def send_tiles(index, level, make):
        count = slots // pieces_far
        for which in range(pieces_far):
            made = [make(rows[odd, which * count + u]) for u in range(count)]
            for u, value in enumerate(made):
                sends[index, 0, which * count + u] = value
            start_far(index, level, which)
        made = [make(rows[1 - odd, u]) for u in range(slots)]
        for u, value in enumerate(made):
            sends[index, 1, u] = value
        start_near(index, level)

    def all_tiles(make, target, begin, count, group=GROUP):
        group = min(group, count)

        @pl.loop(0, count // group)
        def _(i):
            made = [make(begin + i * group + u) for u in range(group)]
            for u in range(group):
                target[begin + i * group + u] = made[u]

    for i, load in enumerate(loads):
        load.wait()

        @pl.loop(0, span // 2)
        def _(j):
            for u in range(2):
                t = i * span + j * 2 + u
                for k in range(nnz):
                    turned[t, k * size : (k + 1) * size] = a_ref[t, k].T

    spread(1)
    wait_halo(0, level0)
    send_tiles(1, level1, first)
    spread(2)
    all_tiles(first, level1, 0, tiles)
    spread(3)
    wait_halo(1, level1)
    half = tiles // 2
    quarter = half // 4
    pieces = [(0, quarter), (quarter, quarter), (2 * quarter, 2 * quarter)]
    pieces = [(0, *piece) for piece in pieces] + [
        (1, 0, half // 2), (1, half // 2, quarter), (1, half // 2 + quarter, quarter)
    ]
    urgent = range(3)
    later = range(3, 6)

    def exchange(c, sender):
        which, offset, count = pieces[c]
        begin = (sender if which == 0 else 1 - sender) * half + offset
        span = pl.ds(begin, count)
        return pltpu.make_async_remote_copy(
            src_ref=level2.at[span],
            dst_ref=other.at[span],
            send_sem=mode_send.at[c],
            recv_sem=mode_recv.at[c],
            device_id=(p, 1 - my),
            device_id_type=MESH,
        )

    def exchanged(c):
        which, offset, count = pieces[c]
        begin = (my if which == 0 else 1 - my) * half + offset
        all_tiles(second, level2, begin, count)
        exchange(c, my).start()

    block = shares.shape[2]
    base = (parts - 8) // 2

    def owners(k):
        return [base + k % 2 + 2 * b for b in range(4)]

    def owned(k):
        place = p - base
        inside = (place >= 0) & (place < 8)
        return inside & (lax.rem(place + parts, 2) == k % 2)

    def blocks_wait(ref, count, sem):
        view = ref.at[pl.ds(0, count)]
        pltpu.make_async_copy(view, view, sem).wait()

    def share(k, value):
        for b, owner in enumerate(owners(k)):
            shares[k, b] = value[b * block : (b + 1) * block]
        for b, owner in enumerate(owners(k)):
            copy = pltpu.make_async_remote_copy(
                src_ref=shares.at[k, b],
                dst_ref=gathered.at[k * parts + p],
                send_sem=share_send.at[k],
                recv_sem=share_recv.at[k],
                device_id=(owner, my),
                device_id_type=MESH,
            )
            pl.when(p != owner)(copy.start)

            @pl.when(p == owner)
            def _():
                gathered[k * parts + p] = shares[k, b]

    def total(k):
        count = len(owners(k))

        @pl.when(owned(k))
        def _():
            blocks_wait(gathered, parts - 1, share_recv.at[k])
            value = gathered[k * parts]
            for q in range(1, parts):
                value = value + gathered[k * parts + q]
            sums[k] = value
            slot = my * count + (p - base) // (8 // count)
            totals[k, slot] = value

            for shift, other_mode in reversed(near_first):
                pltpu.make_async_remote_copy(
                    src_ref=sums.at[k],
                    dst_ref=totals.at[k, slot],
                    send_sem=total_send.at[k],
                    recv_sem=total_recv.at[k],
                    device_id=peer(shift, other_mode),
                    device_id_type=MESH,
                ).start()

    def arrived(k):
        count = len(owners(k))

        @pl.when(owned(k))
        def _():
            blocks_wait(totals.at[k], 2 * count - 1, total_recv.at[k])

        @pl.when(jnp.logical_not(owned(k)))
        def _():
            blocks_wait(totals.at[k], 2 * count, total_recv.at[k])

        flat = totals[k, : 2 * count].reshape(2, count * block, width) / (parts * tiles * size)
        return flat[0], flat[1]

    def sent(k):
        count = len(owners(k))

        @pl.when(owned(k))
        def _():
            blocks_wait(shares.at[k], count - 1, share_send.at[k])
            blocks_wait(gathered, 2 * parts - 1, total_send.at[k])

        @pl.when(jnp.logical_not(owned(k)))
        def _():
            blocks_wait(shares.at[k], count, share_send.at[k])

    def contract(left, right, begin, count):
        acc = jnp.zeros((modes, modes), jnp.float32)
        for i in range(0, count, 8):
            lhs = jnp.concatenate([left[begin + i + u] for u in range(8)], axis=1)
            rhs = jnp.concatenate([right[begin + i + u] for u in range(8)], axis=1)
            acc = acc + lax.dot_general(lhs, rhs, NT, preferred_element_type=jnp.float32)
        return acc

    def fold(value):
        return jnp.concatenate([value[: modes // 2], value[modes // 2 :]], axis=1)

    def unfold(value):
        return jnp.concatenate([value[:, :modes], value[:, modes:]], axis=0)

    for c in urgent:
        exchanged(c)
    spread(4)
    send_tiles(2, level2, second)
    for c in later:
        exchanged(c)
    for stage in range(5, len(partners) + 1):
        spread(stage)
    share(0, fold(contract(level2, level2, 0, tiles)))
    wait_halo(2, level2)
    all_tiles(lambda t: product(level2, t).astype(jnp.bfloat16), image, 0, tiles)
    share(2, fold(contract(image, level2, 0, tiles)))
    for c in urgent:
        exchange(c, 1 - my).wait_recv()
    cross = contract(level2, other, (1 - my) * half, half)
    share(1, fold(jnp.where(my == 0, cross, cross.T)))
    mixed = contract(image, other, (1 - my) * half, half)
    total(0)
    total(1)
    rest_begin = my * half
    exchange(3, 1 - my).wait_recv()
    mixed = mixed + contract(image, other, rest_begin, half // 2)
    for c in (4, 5):
        exchange(c, 1 - my).wait_recv()
    share(3, fold(mixed + contract(image, other, rest_begin + half // 2, half // 2)))

    step = 16
    row_id = lax.broadcasted_iota(jnp.int32, (modes, modes), 0)
    col_id = lax.broadcasted_iota(jnp.int32, (modes, modes), 1)
    small = lax.broadcasted_iota(jnp.int32, (step, 1), 0)
    lanes = lax.broadcasted_iota(jnp.int32, (step, width), 1)

    def exact(left, right, dims):
        return lax.dot_general(
            left, right, dims, precision=EXACT, preferred_element_type=jnp.float32
        )

    def factor_inverse(gram):
        eye = (row_id == col_id).astype(jnp.float32)
        work[...] = jnp.concatenate([gram, eye], axis=1)

        @pl.loop(0, modes // step)
        def _(b):
            begin = pl.multiple_of(b * step, step)
            panel = work[pl.ds(begin, step), :]
            near = panel
            columns = [
                jnp.sum(jnp.where(lanes == begin + s, near, 0.0), axis=1, keepdims=True)
                for s in range(step)
            ]
            pivots = jnp.zeros((step, 1), jnp.float32)
            for q in range(step):
                pivot = columns[q][q : q + 1, :]
                pivots = jnp.where(small == q, pivot, pivots)
                if q == step - 1:
                    break
                factor = jnp.where(small > q, columns[q] / pivot, 0.0)
                panel = panel - factor * panel[q : q + 1, :]
                for s in range(q + 1, step):
                    columns[s] = columns[s] - factor * columns[s][q : q + 1, :]
            inv_ref[pl.ds(begin, step), :] = panel / jnp.sqrt(pivots)
            ahead = (lanes >= begin + step) & (lanes < modes)
            below = jnp.where(ahead, panel / pivots, 0.0)[:, :modes]
            work[...] = work[...] - exact(below, panel, TN)

        return inv_ref[...][:, modes:]

    total(2)
    gram0, gram1 = arrived(0)
    gram0, gram1 = unfold(gram0), unfold(gram1)
    inv00 = factor_inverse(gram0)
    cross0, cross1 = arrived(1)
    bridge = exact(inv00, unfold(cross0 + cross1), NN)
    rest = gram1 - exact(bridge, bridge, TN)
    turn = exact(bridge, inv00, TN)
    total(3)
    inv11 = factor_inverse(rest)
    inv10 = -exact(inv11, turn, NN)
    lower = jnp.concatenate([inv10, inv11], axis=1)
    blank = jnp.zeros((modes, modes), jnp.float32)
    upper = jnp.concatenate([inv00, blank], axis=1)
    inverse = jnp.concatenate([upper, lower], axis=0)
    own = jnp.where(my == 0, upper, pltpu.roll(lower, modes, 1))
    inv_t[...] = own.astype(jnp.bfloat16)
    for t in range(0, tiles, 2):
        two = jnp.concatenate(
            [jnp.concatenate([level2[u], other[u]], axis=0) for u in (t, t + 1)], axis=1
        )
        basis[:, t * size : (t + 2) * size] = lax.dot_general(
            inv_t[...], two, NN, preferred_element_type=jnp.float32
        ).astype(jnp.bfloat16)
    keep = pltpu.make_async_copy(basis, basis_ref, keep_sem.at[0])
    keep.start()
    own0, own1 = arrived(2)
    late0, late1 = arrived(3)
    projected_t = jnp.concatenate(
        [
            jnp.concatenate([unfold(own0), unfold(late0)], axis=1),
            jnp.concatenate([unfold(late1), unfold(own1)], axis=1),
        ],
        axis=0,
    )
    ritz_ref[...] = exact(exact(inverse, projected_t, NT), inverse, NT)
    keep.wait()
    for c in range(chunks):
        exchange(c, my).wait_send()
    for k in range(4):
        sent(k)


def finish(basis_in, ritz_in, basis_ref, ritz_ref, sem):
    copies = [
        pltpu.make_async_copy(basis_in, basis_ref, sem.at[0]),
        pltpu.make_async_copy(ritz_in, ritz_ref, sem.at[1]),
    ]
    for copy in copies:
        copy.start()
    for copy in copies:
        copy.wait()


def shards(parts, stiffness_tiles, tile_cols, send_rows, block, lower_bound, upper_bound):
    row_count, modes = block.shape
    tiles, nnz, size = stiffness_tiles.shape[:3]
    slots = send_rows.shape[1]
    width = 2 * modes
    assert parts >= 16 and parts & (parts - 1) == 0
    chunks = 6
    vmem = pl.BlockSpec(memory_space=pltpu.VMEM)
    hbm = pl.BlockSpec(memory_space=pl.ANY)
    far = pl.BlockSpec(memory_space=pltpu.HBM)
    dma = pltpu.SemaphoreType.DMA
    level = pltpu.VMEM((tiles + 2 * slots, modes, size), jnp.bfloat16)
    field = pltpu.VMEM((tiles, modes, size), jnp.bfloat16)
    basis, ritz = pl.pallas_call(
        functools.partial(kernel, parts),
        out_shape=(
            jax.ShapeDtypeStruct((modes, row_count), jnp.bfloat16),
            jax.ShapeDtypeStruct((width, width), jnp.float32),
        ),
        in_specs=[far] * 6,
        out_specs=(hbm, vmem),
        scratch_shapes=[
            pltpu.VMEM(stiffness_tiles.shape, jnp.bfloat16),
            pltpu.VMEM((tiles, nnz * size, size), jnp.bfloat16),
            level, level, level, pltpu.VMEM((modes, row_count), jnp.bfloat16), field, field, field,
            pltpu.VMEM((3, 2, slots, modes, size), jnp.bfloat16),
            pltpu.VMEM((4, 4, 8, width), jnp.float32),
            pltpu.VMEM((4 * parts, 8, width), jnp.float32),
            pltpu.VMEM((4, 8, 8, width), jnp.float32),
            pltpu.VMEM((4, 8, width), jnp.float32),
            pltpu.VMEM((modes, width), jnp.float32),
            pltpu.VMEM((modes, width), jnp.float32),
            pltpu.VMEM((modes, width), jnp.bfloat16),
            pltpu.VMEM((modes, row_count), jnp.bfloat16),
            pltpu.SMEM((nnz, tiles), jnp.int32),
            pltpu.SMEM(send_rows.shape, jnp.int32),
            pltpu.SMEM((1,), jnp.float32),
            pltpu.SMEM((1,), jnp.float32),
            pltpu.SemaphoreType.REGULAR((parts.bit_length(),)),
            dma((5,)), dma((8,)), dma((1,)), dma((3, 3)), dma((3, 3)), dma((chunks,)), dma((chunks,)),
            dma((4,)), dma((4,)), dma((4,)), dma((4,)),
        ],
        compiler_params=pltpu.CompilerParams(
            collective_id=0, has_side_effects=True, vmem_limit_bytes=50331648
        ),
    )(
        *[pltpu.with_memory_space_constraint(ref, pltpu.HBM) for ref in (tile_cols.T, send_rows)],
        lower_bound, upper_bound,
        *[pltpu.with_memory_space_constraint(ref, pltpu.HBM) for ref in (block.T, stiffness_tiles)],
    )
    basis, ritz = pl.pallas_call(
        finish,
        out_shape=(
            jax.ShapeDtypeStruct((modes, row_count), jnp.bfloat16),
            jax.ShapeDtypeStruct((width, width), jnp.float32),
        ),
        in_specs=[hbm, hbm],
        out_specs=(hbm, hbm),
        scratch_shapes=[dma((2,))],
        compiler_params=pltpu.CompilerParams(vmem_limit_bytes=8 * 1024 * 1024),
    )(basis, ritz)
    return basis.T, ritz


def solution(mesh):
    placed = (
        P("dof", None, None, None),
        P("dof", None),
        P("dof", None),
        P("dof", "mode"),
        P(),
        P(),
    )
    return jax.shard_map(
        functools.partial(shards, mesh.shape["dof"]),
        mesh=mesh, in_specs=placed, out_specs=(P("dof", "mode"), P()), check_vma=False,
    )
```
